8 devices in a mesh: dp: 2 (over z, y), sp: 4 (over x, core).
Axes of the slice: x: 2, y: 2, z: 1, core: 2. Of those that a mesh axis runs over, the one named last changes fastest.
Arguments:
- hidden: bfloat16 [128, 6144], P(('dp', 'sp')), parts along dimension 0
- w_q: bfloat16 [6144, 12288], replicated
- w_k: bfloat16 [6144, 1024], replicated
- w_v: bfloat16 [6144, 1024], replicated
- w_o: bfloat16 [12288, 6144], replicated
- expert_ids: int32 [128, 2], P(('dp', 'sp')), parts along dimension 0
- router_probs: float32 [128, 160], P(('dp', 'sp')), parts along dimension 0
Outputs:
- output 1: bfloat16 [128, 6144], P(('dp', 'sp')), parts along dimension 0
- output 2: bfloat16 [320, 64, 6144], P(('dp', 'sp')), parts along dimension 0
There are 2 independent parts. The reference program is written for one: setup_inputs(seed, part) draws one part's arguments, and reference() takes and returns one part's arrays. A program takes and returns all parts, laid end to end along the dimension named above; an argument that names none is the same for every part.
All inputs are finite; a program needn't handle non-finite values.
Results may differ from the reference program's by a relative error of at most 0.00846543.
Values are sent between devices in bfloat16 or wider.
A program may use at most 1.5 GiB of HBM per device.

```python
import math
import jax
import jax.numpy as jnp
from jax import lax

D = 6144
HEADS = 96
KV_HEADS = 8
HEAD = 128
EXPERTS = 160
TOKENS_DEV = 16
GROUP = 4

SEQ = TOKENS_DEV * GROUP
Q_PER_KV = HEADS // KV_HEADS
Q_WIDTH = HEADS * HEAD
KV_WIDTH = KV_HEADS * HEAD
SCORE_SCALE = 1.0 / math.sqrt(HEAD)


def draw_routes(route_key):
    key_first, key_second, key_pick, key_cold, key_order = jax.random.split(route_key, 5)
    hot_first = jax.random.randint(key_first, (), 0, EXPERTS)
    hot_second = (hot_first + 1 + jax.random.randint(key_second, (), 0, EXPERTS - 1)) % EXPERTS
    pick_hot = jax.random.randint(key_pick, (SEQ,), 0, 2)
    cold_ids = (hot_first + 1 + jax.random.randint(key_cold, (SEQ,), 0, EXPERTS - 1)) % EXPERTS
    other_ids = jnp.where(pick_hot == 1, hot_second, cold_ids)
    first_ids = jnp.full((SEQ,), hot_first)
    swap_bits = jax.random.randint(key_order, (SEQ,), 0, 2)
    col_zero = jnp.where(swap_bits == 1, other_ids, first_ids)
    col_one = jnp.where(swap_bits == 1, first_ids, other_ids)
    return jnp.stack([col_zero, col_one], axis=1).astype(jnp.int32)


def setup_inputs(seed: int = 0, part: int = 0) -> dict:
    base_key = jax.random.key(seed)
    part_key = jax.random.fold_in(base_key, part)
    weight_keys = jax.random.split(base_key, 4)
    part_keys = jax.random.split(part_key, 3)
    q_gain = math.sqrt(0.5 * math.log(SEQ))
    o_gain = 0.5 * SEQ ** 0.25
    hidden = jax.random.normal(part_keys[0], (SEQ, D), jnp.float32).astype(jnp.bfloat16)
    w_q = (jax.random.normal(weight_keys[0], (D, Q_WIDTH), jnp.float32) * (q_gain / math.sqrt(D))).astype(jnp.bfloat16)
    w_k = (jax.random.normal(weight_keys[1], (D, KV_WIDTH), jnp.float32) / math.sqrt(D)).astype(jnp.bfloat16)
    w_v = (jax.random.normal(weight_keys[2], (D, KV_WIDTH), jnp.float32) / math.sqrt(D)).astype(jnp.bfloat16)
    w_o = (jax.random.normal(weight_keys[3], (Q_WIDTH, D), jnp.float32) * (o_gain / math.sqrt(Q_WIDTH))).astype(jnp.bfloat16)
    expert_ids = draw_routes(part_keys[1])
    router_probs = jax.nn.softmax(1.5 * jax.random.normal(part_keys[2], (SEQ, EXPERTS), jnp.float32), axis=1)
    return {'hidden': hidden, 'w_q': w_q, 'w_k': w_k, 'w_v': w_v, 'w_o': w_o, 'expert_ids': expert_ids, 'router_probs': router_probs}


def reference(hidden, w_q, w_k, w_v, w_o, expert_ids, router_probs):
    q_all = jnp.dot(hidden, w_q, preferred_element_type=jnp.float32).astype(jnp.bfloat16)
    k_all = jnp.dot(hidden, w_k, preferred_element_type=jnp.float32).astype(jnp.bfloat16)
    v_all = jnp.dot(hidden, w_v, preferred_element_type=jnp.float32).astype(jnp.bfloat16)
    q_groups = q_all.reshape(SEQ, KV_HEADS, Q_PER_KV, HEAD).transpose(1, 0, 2, 3)
    k_groups = k_all.reshape(SEQ, KV_HEADS, HEAD).transpose(1, 0, 2)
    v_groups = v_all.reshape(SEQ, KV_HEADS, HEAD).transpose(1, 0, 2)
    positions = jnp.arange(SEQ)
    causal = positions[:, None] >= positions[None, :]

    def one_group(group_in):
        q_grp, k_grp, v_grp = group_in
        scores = jnp.einsum('qmd,kd->mqk', q_grp.astype(jnp.float32), k_grp.astype(jnp.float32)) * SCORE_SCALE
        scores = jnp.where(causal[None, :, :], scores, -1e30)
        weights = jax.nn.softmax(scores, axis=-1).astype(jnp.bfloat16)
        out_grp = jnp.einsum('mqk,kd->qmd', weights.astype(jnp.float32), v_grp.astype(jnp.float32))
        return out_grp.astype(jnp.bfloat16)

    attn_out = lax.map(one_group, (q_groups, k_groups, v_groups))
    attn_out = attn_out.transpose(1, 0, 2, 3).reshape(SEQ, Q_WIDTH)
    out_proj = jnp.dot(attn_out, w_o, preferred_element_type=jnp.float32)
    hidden_out = (hidden.astype(jnp.float32) + out_proj).astype(jnp.bfloat16)
    picked = jnp.take_along_axis(router_probs, expert_ids, axis=1)
    gate_w = picked / jnp.sum(picked, axis=1, keepdims=True)
    gated = (gate_w[:, :, None] * hidden_out.astype(jnp.float32)[:, None, :]).astype(jnp.bfloat16)
    ids_blk = expert_ids.reshape(GROUP, TOKENS_DEV, 2)
    token_hits = jnp.sum((ids_blk[:, :, :, None] == jnp.arange(EXPERTS)).astype(jnp.int32), axis=2)
    earlier = jnp.cumsum(token_hits, axis=1) - token_hits
    slot_rank = jnp.take_along_axis(earlier, ids_blk, axis=2)
    dest_rows = jnp.arange(GROUP)[:, None, None] * TOKENS_DEV + slot_rank
    buffer = jnp.zeros((EXPERTS, GROUP * TOKENS_DEV, D), jnp.bfloat16)
    buffer = buffer.at[ids_blk, dest_rows].set(gated.reshape(GROUP, TOKENS_DEV, 2, D))
    return (hidden_out, buffer)
```

```python
import functools
import math
import jax
import jax.numpy as jnp
from jax import lax
from jax.experimental import pallas as pl
from jax.experimental.pallas import tpu as pltpu
from jax.sharding import PartitionSpec as P

HEAD_DIM = 128
SCORE_SCALE = 1.0 / math.sqrt(HEAD_DIM)
SLOTS = 10
BLOCKS = 8
MESH = pl.DeviceIdType.MESH
ANY = pl.BlockSpec(memory_space=pl.ANY)
VMEM = pl.BlockSpec(memory_space=pltpu.VMEM)
SMEM = pl.BlockSpec(memory_space=pltpu.SMEM)


def peer_of(me, mask):
    chip = lax.rem(me // 2 + mask // 2, 2)
    core = lax.rem(lax.rem(me, 2) + mask % 2, 2)
    return chip * 2 + core


def attend_kernel(x_hbm, wq_hbm, wk_hbm, wv_hbm, wo_hbm, ids_ref, probs_ref, h_ref, meta_ref,
                  ring, wk_buf, wv_buf, x_all, o_all, m_all, acc, k_acc, v_acc,
                  w_sem, kv_sem, xl_sem, xs_snd, xs_rcv, xd_snd, xd_rcv, xf_snd, xf_rcv,
                  os_snd, os_rcv, od_snd, od_rcv, of_snd, of_rcv, m_snd, m_rcv):
    me = lax.axis_index('sp')
    tok = x_hbm.shape[0]
    seq = x_all.shape[1]
    wide = ring.shape[2]
    steps = x_all.shape[0]
    kv_w = wk_buf.shape[1]
    heads = wide // HEAD_DIM

    def weight_copy(src, slot):
        return pltpu.make_async_copy(src, ring.at[slot], w_sem.at[slot])

    def q_copy(kv, step, slot):
        rows = pl.ds(pl.multiple_of(step * wide, wide), wide)
        cols = pl.ds(pl.multiple_of((me * 2 + kv) * wide, wide), wide)
        return weight_copy(wq_hbm.at[rows, cols], slot)

    def o_copy(j, slot):
        dev = lax.rem(me // 2 + (j % 4) // 2, 2) * 2 + lax.rem(lax.rem(me, 2) + j % 2, 2)
        rows = pl.ds(pl.multiple_of((dev * 2 + j // 4) * wide, wide), wide)
        cols = pl.ds(pl.multiple_of(me * wide, wide), wide)
        return weight_copy(wo_hbm.at[rows, cols], slot)

    kv_cols = pl.ds(pl.multiple_of(me * kv_w, kv_w), kv_w)
    k_copy = pltpu.make_async_copy(wk_hbm.at[:, kv_cols], wk_buf, kv_sem.at[0])
    v_copy = pltpu.make_async_copy(wv_hbm.at[:, kv_cols], wv_buf, kv_sem.at[1])
    q_copy(0, 0, 0).start()
    k_copy.start()
    v_copy.start()
    for n in range(1, 8):
        q_copy(n // 4, n % 4, n).start()
    for n in range(8, SLOTS):
        o_copy(n - 8, n).start()

    mine = pl.ds(pl.multiple_of(me * tok, tok), tok)
    core_mate = peer_of(me, 1)
    chip_mate = peer_of(me, 2)

    def x_local(step):
        cols = pl.ds(pl.multiple_of(step * wide, wide), wide)
        return pltpu.make_async_copy(x_hbm.at[:, cols], x_all.at[step, mine], xl_sem.at[step])

    def x_send(step, to, snd, rcv):
        cols = pl.ds(pl.multiple_of(step * wide, wide), wide)
        return pltpu.make_async_remote_copy(
            src_ref=x_hbm.at[:, cols], dst_ref=x_all.at[step, mine], send_sem=snd.at[step],
            recv_sem=rcv.at[step], device_id={'sp': to}, device_id_type=MESH)

    def x_forward(step):
        theirs = pl.ds(pl.multiple_of(chip_mate * tok, tok), tok)
        return pltpu.make_async_remote_copy(
            src_ref=x_all.at[step, theirs], dst_ref=x_all.at[step, theirs], send_sem=xf_snd.at[step],
            recv_sem=xf_rcv.at[step], device_id={'sp': core_mate}, device_id_type=MESH)

    def o_send(slot, kv, to, snd, rcv):
        return pltpu.make_async_remote_copy(
            src_ref=o_all.at[slot], dst_ref=o_all.at[slot], send_sem=snd.at[kv],
            recv_sem=rcv.at[kv], device_id={'sp': to}, device_id_type=MESH)

    def m_send(mask):
        return pltpu.make_async_remote_copy(
            src_ref=m_all.at[mine], dst_ref=m_all.at[mine], send_sem=m_snd.at[mask],
            recv_sem=m_rcv.at[mask], device_id={'sp': peer_of(me, mask)}, device_id_type=MESH)

    for step in range(steps):
        x_local(step).start()
    barrier = pltpu.get_barrier_semaphore()
    for mask in (1, 2, 3):
        pl.semaphore_signal(barrier, inc=1, device_id={'sp': peer_of(me, mask)}, device_id_type=MESH)
    pl.semaphore_wait(barrier, 3)
    for step in range(steps):
        x_send(step, chip_mate, xs_snd, xs_rcv).start()
        x_send(step, core_mate, xd_snd, xd_rcv).start()

    ids = ids_ref[...]
    probs = probs_ref[...]
    lanes = lax.broadcasted_iota(jnp.int32, probs.shape, 1)
    p0 = jnp.sum(jnp.where(lanes == ids[:, 0:1], probs, 0.0), axis=1, keepdims=True)
    p1 = jnp.sum(jnp.where(lanes == ids[:, 1:2], probs, 0.0), axis=1, keepdims=True)
    total = p0 + p1
    cols = lax.broadcasted_iota(jnp.int32, (tok, HEAD_DIM), 1)
    fids = ids.astype(jnp.float32)
    meta = jnp.where(cols == 0, fids[:, 0:1], jnp.where(cols == 1, fids[:, 1:2],
           jnp.where(cols == 2, p0 / total, jnp.where(cols == 3, p1 / total, 0.0))))
    m_all[mine, :] = meta
    for mask in (1, 2, 3):
        m_send(mask).start()

    acc[...] = jnp.zeros_like(acc)
    k_acc[...] = jnp.zeros_like(k_acc)
    v_acc[...] = jnp.zeros_like(v_acc)

    def first_step(step, carry):
        x_send(step, chip_mate, xs_snd, xs_rcv).wait_recv()
        x_forward(step).start()
        x_local(step).wait()
        x_send(step, core_mate, xd_snd, xd_rcv).wait_recv()
        x_forward(step).wait_recv()

        @pl.when(step == 0)
        def _():
            k_copy.wait()
            v_copy.wait()

        x = x_all[step]
        rows = pl.ds(pl.multiple_of(step * wide, wide), wide)
        k_acc[...] += jnp.dot(x, wk_buf[rows, :], preferred_element_type=jnp.float32)
        v_acc[...] += jnp.dot(x, wv_buf[rows, :], preferred_element_type=jnp.float32)
        q_copy(0, step, step).wait()
        acc[...] += jnp.dot(x, ring[step], preferred_element_type=jnp.float32)
        o_copy(step + SLOTS - 8, step).start()
        return carry

    def second_step(step, carry):
        q_copy(1, step, 4 + step).wait()
        acc[...] += jnp.dot(x_all[step], ring[4 + step], preferred_element_type=jnp.float32)

        @pl.when(step < 12 - SLOTS)
        def _():
            o_copy(step + SLOTS - 4, 4 + step).start()
        return carry

    def attention(kv):
        q = acc[...].astype(jnp.bfloat16)
        k = k_acc[:, kv * HEAD_DIM:(kv + 1) * HEAD_DIM].astype(jnp.bfloat16)
        v = v_acc[:, kv * HEAD_DIM:(kv + 1) * HEAD_DIM].astype(jnp.bfloat16)
        q = jnp.concatenate([q[:, m * HEAD_DIM:(m + 1) * HEAD_DIM] for m in range(heads)], axis=0)
        s = lax.dot_general(q, k, (((1,), (1,)), ((), ())), preferred_element_type=jnp.float32) * SCORE_SCALE
        row = lax.rem(lax.broadcasted_iota(jnp.int32, s.shape, 0), seq)
        s = jnp.where(row >= lax.broadcasted_iota(jnp.int32, s.shape, 1), s, -1e30)
        e = jnp.exp(s - jnp.max(s, axis=1, keepdims=True))
        w = (e / jnp.sum(e, axis=1, keepdims=True)).astype(jnp.bfloat16)
        o = jnp.dot(w, v, preferred_element_type=jnp.float32).astype(jnp.bfloat16)
        slot = me * 2 + kv
        for m in range(heads):
            o_all[slot, :, m * HEAD_DIM:(m + 1) * HEAD_DIM] = o[m * seq:(m + 1) * seq]
        o_send(slot, kv, chip_mate, os_snd, os_rcv).start()
        o_send(slot, kv, core_mate, od_snd, od_rcv).start()

    lax.fori_loop(0, steps, first_step, 0)
    attention(0)
    acc[...] = jnp.zeros_like(acc)
    lax.fori_loop(0, steps, second_step, 0)
    attention(1)
    acc[...] = jnp.zeros_like(acc)

    def out_step(j, carry):
        kv = j // 4
        mask = lax.rem(j, 4)
        far = chip_mate * 2 + kv

        @pl.when(mask == 1)
        def _():
            o_send(far, kv, core_mate, od_snd, od_rcv).wait_recv()

        @pl.when(mask == 2)
        def _():
            o_send(far, kv, chip_mate, os_snd, os_rcv).wait_recv()
            o_send(far, kv, core_mate, of_snd, of_rcv).start()

        @pl.when(mask == 3)
        def _():
            o_send(far, kv, core_mate, of_snd, of_rcv).wait_recv()

        slot = lax.rem(8 + j, SLOTS)
        dev = lax.rem(me // 2 + mask // 2, 2) * 2 + lax.rem(lax.rem(me, 2) + lax.rem(mask, 2), 2)
        o_copy(0, slot).wait()
        acc[...] += jnp.dot(o_all[dev * 2 + kv], ring[slot], preferred_element_type=jnp.float32)
        return carry

    lax.fori_loop(0, 8, out_step, 0)
    h_ref[...] = (x_all[me].astype(jnp.float32) + acc[...]).astype(jnp.bfloat16)

    for mask in (1, 2, 3):
        m_send(mask).wait()
    meta_ref[...] = m_all[...]
    for step in range(steps):
        x_send(step, chip_mate, xs_snd, xs_rcv).wait_send()
        x_send(step, core_mate, xd_snd, xd_rcv).wait_send()
        x_forward(step).wait_send()
    for kv in range(2):
        o_send(0, kv, chip_mate, os_snd, os_rcv).wait_send()
        o_send(0, kv, core_mate, od_snd, od_rcv).wait_send()
        o_send(0, kv, core_mate, of_snd, of_rcv).wait_send()


def attend(x, w_q, w_k, w_v, w_o, ids, probs, group):
    tok, width = x.shape
    seq = tok * group
    kv_w = w_k.shape[1] // group
    kv_dev = kv_w // HEAD_DIM
    wide = w_q.shape[1] // group // kv_dev
    steps = width // wide
    f32, bf16 = jnp.float32, jnp.bfloat16
    dma = pltpu.SemaphoreType.DMA
    assert wide * group == width and kv_dev == 2 and group == 4
    return pl.pallas_call(
        attend_kernel,
        out_shape=(jax.ShapeDtypeStruct((seq, wide), bf16), jax.ShapeDtypeStruct((seq, HEAD_DIM), f32)),
        in_specs=[ANY] * 5 + [VMEM] * 2,
        out_specs=(VMEM, VMEM),
        scratch_shapes=[
            pltpu.VMEM((SLOTS, wide, wide), bf16),
            pltpu.VMEM((width, kv_w), bf16),
            pltpu.VMEM((width, kv_w), bf16),
            pltpu.VMEM((steps, seq, wide), bf16),
            pltpu.VMEM((group * 2, seq, wide), bf16),
            pltpu.VMEM((seq, HEAD_DIM), f32),
            pltpu.VMEM((seq, wide), f32),
            pltpu.VMEM((seq, kv_w), f32),
            pltpu.VMEM((seq, kv_w), f32),
            dma((SLOTS,)), dma((2,)), dma((steps,)),
        ] + [dma((steps,))] * 6 + [dma((2,))] * 6 + [dma((4,))] * 2,
        compiler_params=pltpu.CompilerParams(
            collective_id=0, has_side_effects=True, vmem_limit_bytes=66_000_000),
        cost_estimate=pl.CostEstimate(flops=seq * 2 * width * wide * 4, bytes_accessed=82_000_000, transcendentals=0),
        name='attend',
    )(x, w_q, w_k, w_v, w_o, ids, probs)


def zero_kernel(meta_smem, meta_ref, buf_hbm, list_ref, prep_ref, zero, flag, sem):
    me = lax.axis_index('sp')
    experts = buf_hbm.shape[0]
    seq = meta_ref.shape[0]
    tok = seq // 4
    zero[...] = jnp.zeros_like(zero)

    def fill(e):
        return pltpu.make_async_copy(zero, buf_hbm.at[e], sem.at[e])

    lax.fori_loop(0, experts, lambda e, c: (fill(e).start(), c)[1], 0)

    meta = meta_ref[...]
    rows = meta.T
    t_col = lax.broadcasted_iota(jnp.int32, (seq, seq), 0)
    t_row = lax.broadcasted_iota(jnp.int32, (seq, seq), 1)
    before = (t_col < t_row) & (t_col // tok == t_row // tok)
    source = (lax.broadcasted_iota(jnp.int32, (1, seq), 1) // tok).astype(jnp.float32)
    for k in range(2):
        same = (meta[:, 0:1] == rows[k:k + 1, :]) | (meta[:, 1:2] == rows[k:k + 1, :])
        rank = jnp.sum(jnp.where(before & same, 1.0, 0.0), axis=0, keepdims=True)
        prep_ref[k:k + 1, :] = (rows[k:k + 1, :] * 4.0 + source) * tok + rank
    prep_ref[2:4, :] = rows[2:4, :]

    def clear(i, c):
        flag[i] = 0
        return c

    lax.fori_loop(0, experts * 4 + 1, clear, 0)

    def visit(p, count):
        t = p // 2
        e = meta_smem[t, lax.rem(p, 2)].astype(jnp.int32) - me * experts
        inside = (e >= 0) & (e < experts)
        b = jnp.where(inside, e * 4 + t // tok, experts * 4)
        fresh = inside & (flag[b] == 0)

        @pl.when(fresh)
        def _():
            flag[b] = 1
            list_ref[count] = b
        return count + fresh.astype(jnp.int32)

    list_ref[2 * seq] = lax.fori_loop(0, 2 * seq, visit, 0)
    lax.fori_loop(0, experts, lambda e, c: (fill(e).wait(), c)[1], 0)


def zero_fill(meta, experts, width):
    seq = meta.shape[0]
    return pl.pallas_call(
        zero_kernel,
        out_shape=(jax.ShapeDtypeStruct((experts, seq, width), jnp.bfloat16),
                   jax.ShapeDtypeStruct((2 * seq + 8,), jnp.int32),
                   jax.ShapeDtypeStruct((8, seq), jnp.float32)),
        in_specs=[SMEM, VMEM],
        out_specs=(ANY, SMEM, VMEM),
        scratch_shapes=[pltpu.VMEM((seq, width), jnp.bfloat16), pltpu.SMEM((experts * 4 + 8,), jnp.int32),
                        pltpu.SemaphoreType.DMA((experts,))],
        cost_estimate=pl.CostEstimate(flops=8_000_000_000, bytes_accessed=experts * seq * width * 2, transcendentals=0),
        name='zero_fill',
    )(meta, meta)


def rows_kernel(list_ref, prep_ref, h0, h1, h2, h3, buf_in, buf_hbm, out_ref, stage, sem):
    me = lax.axis_index('sp')
    experts = buf_hbm.shape[0]
    tok = out_ref.shape[0]
    seq, wide = h0.shape
    count = list_ref[2 * seq]
    batches = (count + BLOCKS - 1) // BLOCKS
    parts = [(h, pl.ds(pl.multiple_of(peer_of(me, mask) * wide, wide), wide)) for mask, h in enumerate((h0, h1, h2, h3))]
    mine = pl.ds(pl.multiple_of(me * tok, tok), tok)
    for h, cols in parts:
        out_ref[:, cols] = h[mine, :]

    def put(batch, i):
        slot = lax.rem(batch, 2)
        b = list_ref[batch * BLOCKS + i]
        dst = pl.ds(pl.multiple_of(lax.rem(b, 4) * tok, tok), tok)
        return pltpu.make_async_copy(stage.at[slot, pl.ds(i * tok, tok)], buf_hbm.at[b // 4, dst], sem.at[slot, i])

    def drain(batch):
        for i in range(BLOCKS):
            @pl.when(batch * BLOCKS + i < count)
            def _():
                put(batch, i).wait()

    row = lax.broadcasted_iota(jnp.int32, (BLOCKS * tok, 1), 0)

    def batch_step(batch, carry):
        @pl.when(batch >= 2)
        def _():
            drain(batch - 2)

        key = jnp.zeros((BLOCKS * tok, 1), jnp.int32)
        for i in range(BLOCKS):
            key = jnp.where(row // tok == i, list_ref[batch * BLOCKS + i], key)
        key = ((key + me * experts * 4) * tok + lax.rem(row, tok)).astype(jnp.float32)
        hit0 = key == prep_ref[0:1, :]
        hit1 = key == prep_ref[1:2, :]
        gate = jnp.sum(jnp.where(hit0, prep_ref[2:3, :], 0.0) + jnp.where(hit1, prep_ref[3:4, :], 0.0),
                       axis=1, keepdims=True)
        pick = jnp.where(hit0 | hit1, 1.0, 0.0).astype(jnp.bfloat16)
        for h, cols in parts:
            rows = jnp.dot(pick, h[...], preferred_element_type=jnp.float32)
            stage[lax.rem(batch, 2), :, cols] = (gate * rows).astype(jnp.bfloat16)
        for i in range(BLOCKS):
            @pl.when(batch * BLOCKS + i < count)
            def _():
                put(batch, i).start()
        return carry

    lax.fori_loop(0, batches, batch_step, 0)

    @pl.when(batches >= 2)
    def _():
        drain(batches - 2)

    @pl.when(batches >= 1)
    def _():
        drain(batches - 1)


def write_rows(blocks, prep, hs, buf):
    experts, seq, width = buf.shape
    tok = seq // 4
    return pl.pallas_call(
        rows_kernel,
        out_shape=(jax.ShapeDtypeStruct(buf.shape, buf.dtype), jax.ShapeDtypeStruct((tok, width), jnp.bfloat16)),
        in_specs=[SMEM] + [VMEM] * 5 + [ANY],
        out_specs=(ANY, VMEM),
        input_output_aliases={6: 0},
        scratch_shapes=[pltpu.VMEM((2, BLOCKS * tok, width), jnp.bfloat16), pltpu.SemaphoreType.DMA((2, BLOCKS))],
        cost_estimate=pl.CostEstimate(flops=2_000_000_000, bytes_accessed=4_000_000, transcendentals=0),
        name='write_rows',
    )(blocks, prep, *hs, buf)


def solution(mesh):
    group = mesh.shape['sp']
    row_spec = P(('dp', 'sp'), None)
    buf_spec = P(('dp', 'sp'), None, None)

    def device_step(x_loc, w_q, w_k, w_v, w_o, ids_loc, probs_loc):
        experts = probs_loc.shape[1] // group
        h0, meta = attend(x_loc, w_q, w_k, w_v, w_o, ids_loc, probs_loc, group)
        swap = lambda mask: [(i, i ^ mask) for i in range(group)]
        h2 = lax.ppermute(h0, 'sp', swap(2))
        h1 = lax.ppermute(h0, 'sp', swap(1))
        h3 = lax.ppermute(h0, 'sp', swap(3))
        buf, blocks, prep = zero_fill(meta, experts, x_loc.shape[1])
        buf, hidden_out = write_rows(blocks, prep, (h0, h1, h2, h3), buf)
        return hidden_out, buf

    return jax.shard_map(device_step, mesh=mesh, in_specs=(row_spec, P(), P(), P(), P(), row_spec, row_spec), out_specs=(row_spec, buf_spec), check_vma=False)
```

```python
import math
import jax
import jax.numpy as jnp
from jax import lax
from jax.experimental import pallas as pl
from jax.experimental.pallas import tpu as pltpu
from jax.sharding import PartitionSpec as P

HEAD_DIM = 128
SCORE_SCALE = 1.0 / math.sqrt(HEAD_DIM)
SLOTS = 10
PARTS = ((0, 768), (768, 512), (1280, 256))
BLOCKS = 8
OCC = 256
EARLY = 4
MESH = pl.DeviceIdType.MESH
ANY = pl.BlockSpec(memory_space=pl.ANY)
VMEM = pl.BlockSpec(memory_space=pltpu.VMEM)
SMEM = pl.BlockSpec(memory_space=pltpu.SMEM)
F32, BF16 = jnp.float32, jnp.bfloat16


def peer_of(me, mask):
    chip = lax.rem(me // 2 + mask // 2, 2)
    core = lax.rem(lax.rem(me, 2) + mask % 2, 2)
    return chip * 2 + core


def span(start, size):
    return pl.ds(pl.multiple_of(start, size), size)


def dot(a, b):
    return jnp.dot(a, b, preferred_element_type=F32)


def attend_kernel(x_hbm, ids_hbm, probs_hbm, wq_hbm, wk_hbm, wv_hbm, wo_hbm, h_hbm, occ_hbm, prep_hbm,
                  ring, kv_buf, x_all, o_all, m_all, h_all, acc, kv_acc, q_ref, kv_ref, x_ref, ids_ref, probs_ref,
                  occ_ref, prep_ref, w_sem, kv_sem, p_sem, in_sem, out_sem, xs_snd, xs_rcv, xd_snd, xd_rcv, xf_snd, xf_rcv,
                  os_snd, os_rcv, od_snd, od_rcv, of_snd, of_rcv, hs_snd, hs_rcv, hd_snd, hd_rcv, hf_snd, hf_rcv,
                  m_snd, m_rcv):
    me = lax.axis_index('sp')
    tok, width = x_ref.shape
    seq = x_all.shape[0]
    wide = ring.shape[1]
    steps = width // wide
    kv_w = kv_buf.shape[1] // 2
    heads = wide // HEAD_DIM
    experts = probs_ref.shape[1] // 4
    core_mate = peer_of(me, 1)
    chip_mate = peer_of(me, 2)
    mine = span(me * tok, tok)
    theirs = span(chip_mate * tok, tok)

    def q_copy(n):
        return pltpu.make_async_copy(
            wq_hbm.at[span(lax.rem(n, 4) * wide, wide), span((me * 2 + n // 4) * wide, wide)],
            ring.at[span(n * wide, wide)], w_sem.at[n])

    def k_copy(c):
        rows = span(c * wide, wide)
        return pltpu.make_async_copy(wk_hbm.at[rows, span(me * kv_w, kv_w)], kv_buf.at[rows, pl.ds(0, kv_w)], kv_sem.at[0, c])

    def v_copy(c):
        rows = span(c * wide, wide)
        return pltpu.make_async_copy(wv_hbm.at[rows, span(me * kv_w, kv_w)], kv_buf.at[rows, pl.ds(kv_w, kv_w)], kv_sem.at[1, c])

    def o_copy(j):
        slot = (8 + j) % SLOTS
        return pltpu.make_async_copy(
            wo_hbm.at[span(peer_of(me, j) * 2 * wide, wide), span(me * wide, wide)],
            ring.at[pl.ds(slot * wide, wide)], w_sem.at[slot])

    def p_copy(p, r):
        off, size = PARTS[p]
        return pltpu.make_async_copy(
            wo_hbm.at[span((peer_of(me, r) * 2 + 1) * wide, wide), pl.ds(pl.multiple_of(me * wide + off, 256), size)],
            ring.at[pl.ds((2 + r) * wide, wide), pl.ds(off, size)], p_sem.at[p, r])

    def remote(src, dst, snd, rcv, to):
        return pltpu.make_async_remote_copy(src_ref=src, dst_ref=dst, send_sem=snd, recv_sem=rcv,
                                            device_id={'sp': to}, device_id_type=MESH)

    def x_far(c):
        cols = pl.ds(c * wide, wide)
        return remote(x_ref.at[:, cols], x_all.at[mine, cols], xs_snd.at[c], xs_rcv.at[c], chip_mate)

    def x_near(c):
        cols = pl.ds(c * wide, wide)
        return remote(x_ref.at[:, cols], x_all.at[mine, cols], xd_snd.at[c], xd_rcv.at[c], core_mate)

    def x_pass(c):
        cols = pl.ds(c * wide, wide)
        return remote(x_all.at[theirs, cols], x_all.at[theirs, cols], xf_snd.at[c], xf_rcv.at[c], core_mate)

    def o_part(kv, r):
        return o_all.at[kv, :, pl.ds(r * wide, wide)]

    def o_far(kv):
        return remote(o_part(kv, 0), o_part(kv, 2), os_snd.at[kv], os_rcv.at[kv], chip_mate)

    def o_near(kv):
        return remote(o_part(kv, 0), o_part(kv, 1), od_snd.at[kv], od_rcv.at[kv], core_mate)

    def o_pass(kv):
        return remote(o_part(kv, 2), o_part(kv, 3), of_snd.at[kv], of_rcv.at[kv], core_mate)

    def h_part(p, dev):
        off, size = PARTS[p]
        return h_all.at[:, pl.ds(pl.multiple_of(dev * wide + off, 256), size)]

    def h_far(p):
        return remote(h_part(p, me), h_part(p, me), hs_snd.at[p], hs_rcv.at[p], chip_mate)

    def h_near(p):
        return remote(h_part(p, me), h_part(p, me), hd_snd.at[p], hd_rcv.at[p], core_mate)

    def h_pass(p):
        return remote(h_part(p, chip_mate), h_part(p, chip_mate), hf_snd.at[p], hf_rcv.at[p], core_mate)

    def m_send(mask):
        return remote(m_all.at[mine], m_all.at[mine], m_snd.at[mask], m_rcv.at[mask], peer_of(me, mask))

    barrier = pltpu.get_barrier_semaphore()
    for mask in (1, 2, 3):
        pl.semaphore_signal(barrier, inc=1, device_id={'sp': peer_of(me, mask)}, device_id_type=MESH)
    x_in = pltpu.make_async_copy(x_hbm, x_ref, in_sem.at[0])
    ids_in = pltpu.make_async_copy(ids_hbm, ids_ref, in_sem.at[1])
    probs_in = pltpu.make_async_copy(probs_hbm, probs_ref, in_sem.at[2])
    x_in.start()
    ids_in.start()
    probs_in.start()

    def start_first(c, carry):
        q_copy(c).start()
        k_copy(c).start()
        v_copy(c).start()
        return carry

    def start_second(n, carry):
        q_copy(n).start()
        return carry

    lax.fori_loop(0, 4, start_first, 0)
    lax.fori_loop(4, 8, start_second, 0)
    o_copy(0).start()
    o_copy(1).start()
    x_in.wait()
    pl.semaphore_wait(barrier, 3)
    for c in range(steps):
        x_far(c).start()
        x_near(c).start()
    x_all[mine, :] = x_ref[...]
    ids_in.wait()
    probs_in.wait()
    ids = ids_ref[...].astype(F32)
    probs = probs_ref[...]
    eye = lax.broadcasted_iota(jnp.int32, (tok, tok), 0) == lax.broadcasted_iota(jnp.int32, (tok, tok), 1)
    id0 = jnp.sum(jnp.where(eye, ids[0:1, :], 0.0), axis=1, keepdims=True)
    id1 = jnp.sum(jnp.where(eye, ids[1:2, :], 0.0), axis=1, keepdims=True)
    lanes = lax.broadcasted_iota(jnp.int32, probs.shape, 1).astype(F32)
    p0 = jnp.sum(jnp.where(lanes == id0, probs, 0.0), axis=1, keepdims=True)
    p1 = jnp.sum(jnp.where(lanes == id1, probs, 0.0), axis=1, keepdims=True)
    total = p0 + p1
    cols = lax.broadcasted_iota(jnp.int32, (tok, HEAD_DIM), 1)
    m_all[mine, :] = jnp.where(cols == 0, id0, jnp.where(cols == 1, id1,
                     jnp.where(cols == 2, p0 / total, jnp.where(cols == 3, p1 / total, 0.0))))
    for mask in (1, 2, 3):
        m_send(mask).start()
    def first_dots(c):
        x_near(c).wait_recv()
        x_pass(c).wait_recv()
        k_copy(c).wait()
        v_copy(c).wait()
        x = x_all[:, c * wide:(c + 1) * wide]
        part = dot(x, kv_buf[c * wide:(c + 1) * wide, :])
        if c == 0:
            kv_acc[...] = part
        else:
            kv_acc[...] += part
        q_copy(c).wait()
        part = dot(x, ring[c * wide:(c + 1) * wide, :])
        if c == 0:
            acc[...] = part
        else:
            acc[...] += part

    for c in range(steps):
        x_far(c).wait_recv()
        x_pass(c).start()
        if c > 0:
            first_dots(c - 1)
    first_dots(steps - 1)

    def attention(kv):
        k = kv_ref[:, kv * HEAD_DIM:(kv + 1) * HEAD_DIM]
        v = kv_ref[:, kv_w + kv * HEAD_DIM:kv_w + (kv + 1) * HEAD_DIM]
        q = jnp.concatenate([q_ref[:, m * HEAD_DIM:(m + 1) * HEAD_DIM] for m in range(heads)], axis=0)
        s = lax.dot_general(q, k, (((1,), (1,)), ((), ())), preferred_element_type=F32) * SCORE_SCALE
        row = lax.rem(lax.broadcasted_iota(jnp.int32, s.shape, 0), seq)
        s = jnp.where(row >= lax.broadcasted_iota(jnp.int32, s.shape, 1), s, -1e30)
        e = jnp.exp(s - jnp.max(s, axis=1, keepdims=True))
        w = (e / jnp.sum(e, axis=1, keepdims=True)).astype(BF16)
        o = dot(w, v).astype(BF16)
        for m in range(heads):
            o_all[kv, :, m * HEAD_DIM:(m + 1) * HEAD_DIM] = o[m * seq:(m + 1) * seq]
        o_far(kv).start()
        o_near(kv).start()

    kv_ref[...] = kv_acc[...].astype(BF16)
    q_ref[...] = acc[...].astype(BF16)
    o_copy(2).start()
    o_copy(3).start()
    p_copy(0, 0).start()
    p_copy(0, 1).start()
    attention(0)

    q_copy(4).wait()
    q_copy(5).wait()
    acc[...] = dot(x_all[:, :2 * wide], ring[4 * wide:6 * wide, :])
    p_copy(0, 2).start()
    p_copy(0, 3).start()
    q_copy(6).wait()
    q_copy(7).wait()
    q_ref[...] = (acc[...] + dot(x_all[:, 2 * wide:], ring[6 * wide:8 * wide, :])).astype(BF16)
    for r in range(4):
        p_copy(1, r).start()
    attention(1)

    def routing():
        for mask in (1, 2, 3):
            m_send(mask).wait_recv()
        meta = m_all[...]
        rows = meta.T
        t_col = lax.broadcasted_iota(jnp.int32, (seq, seq), 0)
        t_row = lax.broadcasted_iota(jnp.int32, (seq, seq), 1)
        before = (t_col < t_row) & (t_col // tok == t_row // tok)
        source = (lax.broadcasted_iota(jnp.int32, (1, seq), 1) // tok).astype(F32)
        for k in range(2):
            same = (meta[:, 0:1] == rows[k:k + 1, :]) | (meta[:, 1:2] == rows[k:k + 1, :])
            rank = jnp.sum(jnp.where(before & same, 1.0, 0.0), axis=0, keepdims=True)
            prep_ref[k:k + 1, :] = (rows[k:k + 1, :] * 4.0 + source) * tok + rank
        prep_ref[2:4, :] = rows[2:4, :]
        prep_ref[4:8, :] = jnp.zeros((4, seq), F32)
        block = (lax.broadcasted_iota(jnp.int32, (seq, OCC), 1) + me * experts * 4).astype(F32)
        origin = (lax.broadcasted_iota(jnp.int32, (seq, 1), 0) // tok).astype(F32)
        used = (meta[:, 0:1] * 4.0 + origin == block) | (meta[:, 1:2] * 4.0 + origin == block)
        occ_ref[...] = jnp.max(jnp.where(used, 1, 0), axis=0, keepdims=True)
        occ_out = pltpu.make_async_copy(occ_ref, occ_hbm, out_sem.at[0])
        prep_out = pltpu.make_async_copy(prep_ref, prep_hbm, out_sem.at[1])
        occ_out.start()
        prep_out.start()
        return occ_out, prep_out

    for r in range(4):
        if r == 1:
            o_near(0).wait_recv()
            occ_out, prep_out = routing()
        if r == 2:
            o_far(0).wait_recv()
            o_pass(0).start()
        if r == 3:
            o_pass(0).wait_recv()
        o_copy(r).wait()
        if r == 0:
            for s in range(4):
                p_copy(2, s).start()
        slot = (8 + r) % SLOTS
        part = dot(o_all[0, :, r * wide:(r + 1) * wide], ring[slot * wide:(slot + 1) * wide, :])
        if r == 0:
            acc[...] = part
        else:
            acc[...] += part

    for p, (off, size) in enumerate(PARTS):
        cut = slice(off, off + size)
        if p == 0:
            o_near(1).wait_recv()
        p_copy(p, 0).wait()
        p_copy(p, 1).wait()
        part = dot(o_all[1, :, :2 * wide], ring[2 * wide:4 * wide, cut])
        acc[:, cut] += part
        if p == 0:
            o_far(1).wait_recv()
            o_pass(1).start()
            p_copy(p, 2).wait()
            part = dot(o_all[1, :, 2 * wide:3 * wide], ring[4 * wide:5 * wide, cut])
            acc[:, cut] += part
            o_pass(1).wait_recv()
            p_copy(p, 3).wait()
            part = dot(o_all[1, :, 3 * wide:], ring[5 * wide:6 * wide, cut])
        else:
            p_copy(p, 2).wait()
            p_copy(p, 3).wait()
            part = dot(o_all[1, :, 2 * wide:], ring[4 * wide:6 * wide, cut])
        home = pl.ds(pl.multiple_of(me * wide + off, 256), size)
        h_all[:, home] = (x_all[:, home].astype(F32) + (acc[:, cut] + part)).astype(BF16)
        h_far(p).start()
        h_near(p).start()

    last = PARTS[-1][0]

    def h_out(dev, off, size, sem):
        cut = pl.ds(dev * wide + off, size)
        return pltpu.make_async_copy(h_all.at[:, cut], h_hbm.at[:, cut], sem)

    for p in range(len(PARTS)):
        h_far(p).wait_recv()
        h_pass(p).start()
        if p > 0:
            h_near(p - 1).wait_recv()
            h_pass(p - 1).wait_recv()
    for dev in range(4):
        h_out(dev, 0, last, out_sem.at[2 + dev]).start()
    h_near(len(PARTS) - 1).wait_recv()
    h_pass(len(PARTS) - 1).wait_recv()
    for dev in range(4):
        h_out(dev, last, wide - last, out_sem.at[6 + dev]).start()
    for mask in (1, 2, 3):
        m_send(mask).wait_send()
    for c in range(steps):
        x_far(c).wait_send()
        x_near(c).wait_send()
        x_pass(c).wait_send()
    for kv in range(2):
        o_far(kv).wait_send()
        o_near(kv).wait_send()
        o_pass(kv).wait_send()
    for p in range(len(PARTS)):
        h_far(p).wait_send()
        h_near(p).wait_send()
        h_pass(p).wait_send()
    occ_out.wait()
    prep_out.wait()
    for dev in range(4):
        h_out(dev, 0, last, out_sem.at[2 + dev]).wait()
        h_out(dev, last, wide - last, out_sem.at[6 + dev]).wait()


def attend(x, ids_t, probs, w_q, w_k, w_v, w_o, group):
    tok, width = x.shape
    seq = tok * group
    kv_w = w_k.shape[1] // group
    kv_dev = kv_w // HEAD_DIM
    wide = w_q.shape[1] // group // kv_dev
    steps = width // wide
    dma = pltpu.SemaphoreType.DMA
    parts = len(PARTS)
    assert steps == 4 and kv_dev == 2 and group == 4
    return pl.pallas_call(
        attend_kernel,
        out_shape=(jax.ShapeDtypeStruct((seq, width), BF16), jax.ShapeDtypeStruct((1, OCC), jnp.int32),
                   jax.ShapeDtypeStruct((8, seq), F32)),
        in_specs=[ANY] * 7,
        out_specs=(ANY, ANY, ANY),
        scratch_shapes=[
            pltpu.VMEM((SLOTS * wide, wide), BF16),
            pltpu.VMEM((width, 2 * kv_w), BF16),
            pltpu.VMEM((seq, width), BF16),
            pltpu.VMEM((2, seq, group * wide), BF16),
            pltpu.VMEM((seq, HEAD_DIM), F32),
            pltpu.VMEM((seq, width), BF16),
            pltpu.VMEM((seq, wide), F32),
            pltpu.VMEM((seq, 2 * kv_w), F32),
            pltpu.VMEM((seq, wide), BF16),
            pltpu.VMEM((seq, 2 * kv_w), BF16),
            pltpu.VMEM(x.shape, BF16), pltpu.VMEM(ids_t.shape, jnp.int32), pltpu.VMEM(probs.shape, F32),
            pltpu.VMEM((1, OCC), jnp.int32), pltpu.VMEM((8, seq), F32),
            dma((SLOTS,)), dma((2, steps)), dma((parts, 4)), dma((3,)), dma((10,)),
        ] + [dma((steps,))] * 6 + [dma((2,))] * 6 + [dma((parts,))] * 6 + [dma((4,))] * 2,
        compiler_params=pltpu.CompilerParams(
            collective_id=0, has_side_effects=True, vmem_limit_bytes=66_000_000),
        cost_estimate=pl.CostEstimate(flops=seq * 2 * width * wide * 4, bytes_accessed=82_000_000, transcendentals=0),
        name='attend',
    )(x, ids_t, probs, w_q, w_k, w_v, w_o)


def dispatch_kernel(occ_hbm, prep_hbm, h_hbm, buf_hbm, out_hbm, occ_ref, h, prep_ref, zero, stage, todo, z_sem, s_sem, io_sem):
    me = lax.axis_index('sp')
    experts = buf_hbm.shape[0]
    tok = out_hbm.shape[0]
    h_copy = pltpu.make_async_copy(h_hbm, h, io_sem.at[0])
    prep_copy = pltpu.make_async_copy(prep_hbm, prep_ref, io_sem.at[1])
    out_copy = pltpu.make_async_copy(h.at[span(me * tok, tok)], out_hbm, io_sem.at[2])
    occ_copy = pltpu.make_async_copy(occ_hbm, occ_ref, io_sem.at[3])
    occ_copy.start()
    h_copy.start()
    prep_copy.start()
    zero[...] = jnp.zeros_like(zero)

    def fill(b):
        return pltpu.make_async_copy(zero.at[pl.ds(0, tok)], buf_hbm.at[b // 4, span(lax.rem(b, 4) * tok, tok)], z_sem.at[b])

    def fill_all(e):
        return pltpu.make_async_copy(zero, buf_hbm.at[e], z_sem.at[e * 4])

    def busy(e):
        return occ_ref[0, e * 4] + occ_ref[0, e * 4 + 1] + occ_ref[0, e * 4 + 2] + occ_ref[0, e * 4 + 3]

    def listed(b, count):
        one = occ_ref[0, b]

        @pl.when(one != 0)
        def _():
            todo[count] = b
        return count + one

    def first(e, count):
        used = busy(e)

        @pl.when(used == 0)
        def _():
            fill_all(e).start()

        @pl.when(used != 0)
        def _():
            at = count
            for i in range(4):
                b = e * 4 + i
                one = occ_ref[0, b]

                @pl.when(one == 0)
                def _():
                    fill(b).start()

                @pl.when(one != 0)
                def _():
                    todo[at] = b
                at = at + one
        return count + used

    for e in range(EARLY):
        fill_all(e).start()
    occ_copy.wait()
    count = lax.fori_loop(0, EARLY * 4, listed, 0)
    count = lax.fori_loop(EARLY, experts, first, count)
    batches = (count + BLOCKS - 1) // BLOCKS

    def put(batch, i):
        slot = lax.rem(batch, 2)
        b = todo[batch * BLOCKS + i]
        return pltpu.make_async_copy(stage.at[slot, pl.ds(i * tok, tok)],
                                     buf_hbm.at[b // 4, span(lax.rem(b, 4) * tok, tok)], s_sem.at[slot, i])

    def drain(batch):
        for i in range(BLOCKS):
            @pl.when(batch * BLOCKS + i < count)
            def _():
                put(batch, i).wait()

    row = lax.broadcasted_iota(jnp.int32, (BLOCKS * tok, 1), 0)
    prep_copy.wait()
    h_copy.wait()
    out_copy.start()
    for e in range(EARLY):
        fill_all(e).wait()

    def batch_step(batch, carry):
        @pl.when(batch >= 2)
        def _():
            drain(batch - 2)

        key = jnp.zeros((BLOCKS * tok, 1), jnp.int32)
        for i in range(BLOCKS):
            key = jnp.where(row // tok == i, todo[batch * BLOCKS + i], key)
        key = ((key + me * experts * 4) * tok + lax.rem(row, tok)).astype(F32)
        hit0 = key == prep_ref[0:1, :]
        hit1 = key == prep_ref[1:2, :]
        gate = jnp.sum(jnp.where(hit0, prep_ref[2:3, :], 0.0) + jnp.where(hit1, prep_ref[3:4, :], 0.0),
                       axis=1, keepdims=True)
        pick = jnp.where(hit0 | hit1, 1.0, 0.0).astype(BF16)
        stage[lax.rem(batch, 2)] = (gate * dot(pick, h[...])).astype(BF16)
        for i in range(BLOCKS):
            @pl.when(batch * BLOCKS + i < count)
            def _():
                put(batch, i).start()
        return carry

    lax.fori_loop(0, batches, batch_step, 0)

    @pl.when(batches >= 2)
    def _():
        drain(batches - 2)

    @pl.when(batches >= 1)
    def _():
        drain(batches - 1)

    def last(e, c):
        used = busy(e)

        @pl.when(used == 0)
        def _():
            fill_all(e).wait()

        @pl.when(used != 0)
        def _():
            for i in range(4):
                @pl.when(occ_ref[0, e * 4 + i] == 0)
                def _():
                    fill(e * 4 + i).wait()
        return c

    lax.fori_loop(EARLY, experts, last, 0)
    out_copy.wait()


def dispatch(occ, prep, h, experts, tok):
    seq, width = h.shape
    dma = pltpu.SemaphoreType.DMA
    return pl.pallas_call(
        dispatch_kernel,
        out_shape=(jax.ShapeDtypeStruct((experts, seq, width), BF16), jax.ShapeDtypeStruct((tok, width), BF16)),
        in_specs=[ANY, ANY, ANY],
        out_specs=(ANY, ANY),
        scratch_shapes=[pltpu.SMEM((1, OCC), jnp.int32), pltpu.VMEM((seq, width), BF16), pltpu.VMEM((8, seq), F32), pltpu.VMEM((seq, width), BF16),
                        pltpu.VMEM((2, BLOCKS * tok, width), BF16), pltpu.SMEM((experts * 4 + BLOCKS,), jnp.int32),
                        dma((experts * 4,)), dma((2, BLOCKS)), dma((4,))],
        compiler_params=pltpu.CompilerParams(vmem_limit_bytes=66_000_000),
        cost_estimate=pl.CostEstimate(flops=8_000_000_000, bytes_accessed=experts * seq * width * 2, transcendentals=0),
        name='dispatch',
    )(occ, prep, h)


def solution(mesh):
    group = mesh.shape['sp']
    row_spec = P(('dp', 'sp'), None)
    buf_spec = P(('dp', 'sp'), None, None)

    def device_step(x_loc, w_q, w_k, w_v, w_o, ids_loc, probs_loc):
        h, occ, prep = attend(x_loc, ids_loc.T, probs_loc, w_q, w_k, w_v, w_o, group)
        buf, hidden_out = dispatch(occ, prep, h, probs_loc.shape[1] // group, x_loc.shape[0])
        return hidden_out, buf

    return jax.shard_map(device_step, mesh=mesh, in_specs=(row_spec, P(), P(), P(), P(), row_spec, row_spec), out_specs=(row_spec, buf_spec), check_vma=False)
```

```python
import math
import jax
import jax.numpy as jnp
from jax import lax
from jax.experimental import pallas as pl
from jax.experimental.pallas import tpu as pltpu
from jax.sharding import PartitionSpec as P

HEAD_DIM = 128
SCORE_SCALE = 1.0 / math.sqrt(HEAD_DIM)
SLOTS = 10
PARTS = ((0, 1024), (1024, 256), (1280, 256))
SEGS = ((0, 1536), (0, 1024), (1024, 512))
EARLY = 4
PLACE = (8, 9, 0, 1, 2, 3, 4, 5)
MESH = pl.DeviceIdType.MESH
ANY = pl.BlockSpec(memory_space=pl.ANY)
VMEM = pl.BlockSpec(memory_space=pltpu.VMEM)
SMEM = pl.BlockSpec(memory_space=pltpu.SMEM)
F32, BF16 = jnp.float32, jnp.bfloat16


def peer_of(me, mask):
    chip = lax.rem(me // 2 + mask // 2, 2)
    core = lax.rem(lax.rem(me, 2) + mask % 2, 2)
    return chip * 2 + core


def span(start, size):
    return pl.ds(pl.multiple_of(start, size), size)


def dot(a, b):
    return jnp.dot(a, b, preferred_element_type=F32)


def attend_kernel(x_hbm, ids_hbm, probs_hbm, wq_hbm, wk_hbm, wv_hbm, wo_hbm, h_hbm, occ_hbm, prep_hbm,
                  ring, kv_buf, x_all, o_all, m_all, h_all, acc, kv_acc, q_ref, kv_ref, x_ref, ids_ref, probs_ref,
                  occ_ref, prep_ref, w_sem, kv_sem, p_sem, in_sem, out_sem, xs_snd, xs_rcv, xd_snd, xd_rcv, xf_snd, xf_rcv,
                  os_snd, os_rcv, od_snd, od_rcv, of_snd, of_rcv, hs_snd, hs_rcv, hd_snd, hd_rcv, hf_snd, hf_rcv, hg_snd,
                  m_snd, m_rcv):
    me = lax.axis_index('sp')
    tok, width = x_ref.shape
    seq = x_all.shape[0]
    wide = ring.shape[1]
    steps = width // wide
    kv_w = kv_buf.shape[1] // 2
    heads = wide // HEAD_DIM
    experts = probs_ref.shape[1] // 4
    core_mate = peer_of(me, 1)
    chip_mate = peer_of(me, 2)
    mine = span(me * tok, tok)
    theirs = span(chip_mate * tok, tok)

    def q_copy(c):
        rows = span(c * wide, wide)
        return pltpu.make_async_copy(wq_hbm.at[rows, span(me * 2 * wide, wide)], ring.at[rows], w_sem.at[c])

    def r_copy(seg, c):
        off, size = SEGS[seg]
        cols = pl.ds(pl.multiple_of((me * 2 + 1) * wide + off, 512), size)
        return pltpu.make_async_copy(wq_hbm.at[span(c * wide, wide), cols],
                                     ring.at[span((c + 4) * wide, wide), pl.ds(off, size)], w_sem.at[2 + 2 * seg + c // 2])

    def r_dot(seg, half):
        off, size = SEGS[seg]
        deep = 2 * wide
        base = 4 * wide + half * deep
        pltpu.make_async_copy(wq_hbm.at[pl.ds(0, deep), pl.ds(0, size)], ring.at[pl.ds(base, deep), pl.ds(off, size)],
                              w_sem.at[2 + 2 * seg + half]).wait()
        return dot(x_all[:, half * deep:(half + 1) * deep], ring[base:base + deep, off:off + size])

    def k_copy(c):
        rows = span(c * wide, wide)
        return pltpu.make_async_copy(wk_hbm.at[rows, span(me * kv_w, kv_w)], kv_buf.at[rows, pl.ds(0, kv_w)], kv_sem.at[c])

    def v_copy(c):
        rows = span(c * wide, wide)
        return pltpu.make_async_copy(wv_hbm.at[rows, span(me * kv_w, kv_w)], kv_buf.at[rows, pl.ds(kv_w, kv_w)], kv_sem.at[c])

    def p_sem_at(p, i):
        return i // 2 if p == 0 else 3 * p + 1 + (i + 2) // 4

    def p_copy(p, i):
        off, size = PARTS[p]
        return pltpu.make_async_copy(
            wo_hbm.at[span((peer_of(me, i % 4) * 2 + i // 4) * wide, wide), pl.ds(pl.multiple_of(me * wide + off, 128), size)],
            ring.at[pl.ds(PLACE[i] * wide, wide), pl.ds(off, size)], p_sem.at[p_sem_at(p, i)])

    def p_dot(p, i, count):
        off, size = PARTS[p]
        tile = ring.at[pl.ds(PLACE[i] * wide, count * wide), pl.ds(off, size)]
        pltpu.make_async_copy(wo_hbm.at[pl.ds(0, count * wide), pl.ds(0, size)], tile, p_sem.at[p_sem_at(p, i)]).wait()
        base = PLACE[i] * wide
        part = dot(o_all[:, i * wide:(i + count) * wide], ring[base:base + count * wide, off:off + size])
        if i == 0:
            acc[:, off:off + size] = part
        else:
            acc[:, off:off + size] += part

    def remote(src, dst, snd, rcv, to):
        return pltpu.make_async_remote_copy(src_ref=src, dst_ref=dst, send_sem=snd, recv_sem=rcv,
                                            device_id={'sp': to}, device_id_type=MESH)

    def x_far(c):
        cols = pl.ds(c * wide, wide)
        return remote(x_ref.at[:, cols], x_all.at[mine, cols], xs_snd, xs_rcv.at[c], chip_mate)

    def x_near(c):
        cols = pl.ds(c * wide, wide)
        return remote(x_ref.at[:, cols], x_all.at[mine, cols], xd_snd, xd_rcv.at[c], core_mate)

    def x_pass(c):
        cols = pl.ds(c * wide, wide)
        return remote(x_all.at[theirs, cols], x_all.at[theirs, cols], xf_snd, xf_rcv.at[c], core_mate)

    def o_part(seg, r):
        off, size = SEGS[seg]
        return o_all.at[:, pl.ds((min(seg, 1) * 4 + r) * wide + off, size)]

    def o_far(seg):
        return remote(o_part(seg, 0), o_part(seg, 2), os_snd, os_rcv.at[seg], chip_mate)

    def o_near(seg):
        return remote(o_part(seg, 0), o_part(seg, 1), od_snd, od_rcv.at[seg], core_mate)

    def o_pass(seg):
        return remote(o_part(seg, 2), o_part(seg, 3), of_snd, of_rcv.at[seg], core_mate)

    def h_part(p, dev):
        off, size = PARTS[p]
        return h_all.at[:, pl.ds(pl.multiple_of(dev * wide + off, 128), size)]

    def h_far(p):
        return remote(h_part(p, me), h_part(p, me), hs_snd, hs_rcv.at[p], chip_mate)

    def h_near(p):
        return remote(h_part(p, me), h_part(p, me), hd_snd, hd_rcv.at[p], core_mate)

    def h_pass(p):
        return remote(h_part(p, chip_mate), h_part(p, chip_mate), hf_snd, hf_rcv.at[p], core_mate)

    def h_diag():
        p = len(PARTS) - 1
        return remote(h_part(p, me), h_part(p, me), hg_snd, hf_rcv.at[p], peer_of(me, 3))

    def m_send(mask):
        return remote(m_all.at[mine], m_all.at[mine], m_snd, m_rcv.at[mask - 1], peer_of(me, mask))

    barrier = pltpu.get_barrier_semaphore()
    for mask in (1, 2, 3):
        pl.semaphore_signal(barrier, inc=1, device_id={'sp': peer_of(me, mask)}, device_id_type=MESH)
    x_in = pltpu.make_async_copy(x_hbm, x_ref, in_sem.at[0])
    ids_in = pltpu.make_async_copy(ids_hbm, ids_ref, in_sem.at[1])
    probs_in = pltpu.make_async_copy(probs_hbm, probs_ref, in_sem.at[2])
    x_in.start()
    ids_in.start()
    probs_in.start()

    def start_first(c, carry):
        q_copy(c).start()
        k_copy(c).start()
        v_copy(c).start()
        return carry

    def start_second(c, carry):
        r_copy(1, c).start()
        return carry

    def start_third(c, carry):
        r_copy(2, c).start()
        return carry

    lax.fori_loop(0, 4, start_first, 0)
    lax.fori_loop(0, 4, start_second, 0)
    lax.fori_loop(0, 4, start_third, 0)
    p_copy(0, 0).start()
    p_copy(0, 1).start()
    x_in.wait()
    pl.semaphore_wait(barrier, 3)
    for c in range(steps):
        x_far(c).start()
        x_near(c).start()
    x_all[mine, :] = x_ref[...]
    ids_in.wait()
    probs_in.wait()
    ids = ids_ref[...].astype(F32)
    probs = probs_ref[...]
    eye = lax.broadcasted_iota(jnp.int32, (tok, tok), 0) == lax.broadcasted_iota(jnp.int32, (tok, tok), 1)
    id0 = jnp.sum(jnp.where(eye, ids[0:1, :], 0.0), axis=1, keepdims=True)
    id1 = jnp.sum(jnp.where(eye, ids[1:2, :], 0.0), axis=1, keepdims=True)
    lanes = lax.broadcasted_iota(jnp.int32, probs.shape, 1).astype(F32)
    p0 = jnp.sum(jnp.where(lanes == id0, probs, 0.0), axis=1, keepdims=True)
    p1 = jnp.sum(jnp.where(lanes == id1, probs, 0.0), axis=1, keepdims=True)
    total = p0 + p1
    cols = lax.broadcasted_iota(jnp.int32, (tok, HEAD_DIM), 1)
    m_all[mine, :] = jnp.where(cols == 0, id0, jnp.where(cols == 1, id1,
                     jnp.where(cols == 2, p0 / total, jnp.where(cols == 3, p1 / total, 0.0))))
    for mask in (1, 2, 3):
        m_send(mask).start()
    def first_dots(c):
        x_near(c).wait_recv()
        x_pass(c).wait_recv()
        rows = pl.ds(c * wide, wide)
        pltpu.make_async_copy(wq_hbm.at[rows, pl.ds(0, 2 * kv_w)], kv_buf.at[rows, :], kv_sem.at[c]).wait()
        x = x_all[:, c * wide:(c + 1) * wide]
        part = dot(x, kv_buf[c * wide:(c + 1) * wide, :])
        if c == 0:
            kv_acc[...] = part
        else:
            kv_acc[...] += part
        q_copy(c).wait()
        part = dot(x, ring[c * wide:(c + 1) * wide, :])
        if c == 0:
            acc[...] = part
        else:
            acc[...] += part

    for c in range(steps):
        x_far(c).wait_recv()
        x_pass(c).start()
        if c > 0:
            first_dots(c - 1)
    first_dots(steps - 1)

    def attention(seg):
        kv = min(seg, 1)
        start, size = SEGS[seg]
        heads = size // HEAD_DIM
        k = kv_ref[:, kv * HEAD_DIM:(kv + 1) * HEAD_DIM]
        v = kv_ref[:, kv_w + kv * HEAD_DIM:kv_w + (kv + 1) * HEAD_DIM]
        cuts = [slice(start + m * HEAD_DIM, start + (m + 1) * HEAD_DIM) for m in range(heads)]
        q = jnp.concatenate([q_ref[:, c] for c in cuts], axis=0)
        s = lax.dot_general(q, k, (((1,), (1,)), ((), ())), preferred_element_type=F32) * SCORE_SCALE
        row = lax.rem(lax.broadcasted_iota(jnp.int32, s.shape, 0), seq)
        s = jnp.where(row >= lax.broadcasted_iota(jnp.int32, s.shape, 1), s, -1e30)
        e = jnp.exp(s - jnp.max(s, axis=1, keepdims=True))
        w = (e / jnp.sum(e, axis=1, keepdims=True)).astype(BF16)
        o = dot(w, v).astype(BF16)
        for m, c in enumerate(cuts):
            o_all[:, kv * 4 * wide + c.start:kv * 4 * wide + c.stop] = o[m * seq:(m + 1) * seq]
        o_far(seg).start()
        o_near(seg).start()

    kv_ref[...] = kv_acc[...].astype(BF16)
    q_ref[...] = acc[...].astype(BF16)
    for i in (2, 3, 4, 5):
        p_copy(0, i).start()
    attention(0)

    mid = SEGS[2][0]
    acc[:, :mid] = r_dot(1, 0)
    q_ref[:, :mid] = (acc[:, :mid] + r_dot(1, 1)).astype(BF16)
    attention(1)
    acc[:, mid:] = r_dot(2, 0)
    p_copy(0, 6).start()
    p_copy(0, 7).start()
    q_ref[:, mid:] = (acc[:, mid:] + r_dot(2, 1)).astype(BF16)
    for i in range(8):
        p_copy(1, i).start()
    attention(2)

    def routing():
        for mask in (1, 2, 3):
            m_send(mask).wait_recv()
        meta = m_all[...]
        rows = meta.T
        t_col = lax.broadcasted_iota(jnp.int32, (seq, seq), 0)
        t_row = lax.broadcasted_iota(jnp.int32, (seq, seq), 1)
        before = (t_col < t_row) & (t_col // tok == t_row // tok)
        source = (lax.broadcasted_iota(jnp.int32, (1, seq), 1) // tok).astype(F32)
        for k in range(2):
            same = (meta[:, 0:1] == rows[k:k + 1, :]) | (meta[:, 1:2] == rows[k:k + 1, :])
            rank = jnp.sum(jnp.where(before & same, 1.0, 0.0), axis=0, keepdims=True)
            prep_ref[k:k + 1, :] = (rows[k:k + 1, :] * 4.0 + source) * tok + rank
        prep_ref[2:4, :] = rows[2:4, :]
        prep_ref[4:8, :] = jnp.zeros((4, seq), F32)
        block = (lax.broadcasted_iota(jnp.int32, (seq, HEAD_DIM), 1) + me * experts).astype(F32)
        used = (meta[:, 0:1] == block) | (meta[:, 1:2] == block)
        occ_ref[...] = jnp.max(jnp.where(used, 1, 0), axis=0, keepdims=True)
        occ_out = pltpu.make_async_copy(occ_ref, occ_hbm, out_sem.at[0])
        prep_out = pltpu.make_async_copy(prep_ref, prep_hbm, out_sem.at[1])
        occ_out.start()
        prep_out.start()
        return occ_out, prep_out

    o_near(0).wait_recv()
    p_dot(0, 0, 2)
    for i in range(8):
        p_copy(2, i).start()
    occ_out, prep_out = routing()
    o_far(0).wait_recv()
    o_pass(0).start()
    o_far(1).wait_recv()
    o_pass(1).start()
    o_pass(0).wait_recv()
    p_dot(0, 2, 2)
    o_near(1).wait_recv()
    o_near(2).wait_recv()
    o_far(2).wait_recv()
    o_pass(2).start()
    p_dot(0, 4, 2)
    o_pass(1).wait_recv()
    o_pass(2).wait_recv()
    p_dot(0, 6, 2)
    for p, (off, size) in enumerate(PARTS):
        if p > 0:
            p_dot(p, 0, 2)
            p_dot(p, 2, 4)
            p_dot(p, 6, 2)
        home = pl.ds(pl.multiple_of(me * wide + off, 128), size)
        h_all[:, home] = (x_all[:, home].astype(F32) + acc[:, off:off + size]).astype(BF16)
        h_far(p).start()
        if p == len(PARTS) - 1:
            h_diag().start()
        h_near(p).start()

    last = PARTS[-1][0]

    def h_out(dev, off, size, sem):
        cut = pl.ds(dev * wide + off, size)
        return pltpu.make_async_copy(h_all.at[:, cut], h_hbm.at[:, cut], sem)

    for p in range(len(PARTS) - 1):
        h_far(p).wait_recv()
        h_pass(p).start()
    for p in range(len(PARTS) - 1):
        h_near(p).wait_recv()
        h_pass(p).wait_recv()
    for dev in range(4):
        h_out(dev, 0, last, out_sem.at[2]).start()
    h_near(len(PARTS) - 1).wait_recv()
    h_far(len(PARTS) - 1).wait_recv()
    h_diag().wait_recv()
    for dev in range(4):
        h_out(dev, last, wide - last, out_sem.at[3]).start()

    remote(m_all.at[pl.ds(0, 3 * tok)], m_all.at[pl.ds(0, 3 * tok)], m_snd, m_rcv.at[0], core_mate).wait_send()
    for snd in (xs_snd, xd_snd, xf_snd):
        remote(x_ref, x_all.at[mine], snd, xs_rcv.at[0], chip_mate).wait_send()
    both = o_all.at[:, pl.ds(0, 2 * wide)]
    for snd in (os_snd, od_snd, of_snd):
        remote(both, both, snd, os_rcv.at[0], chip_mate).wait_send()
    whole = h_all.at[:, pl.ds(0, wide)]
    for snd in (hs_snd, hd_snd):
        remote(whole, whole, snd, hs_rcv.at[0], chip_mate).wait_send()
    most = h_all.at[:, pl.ds(0, last)]
    remote(most, most, hf_snd, hf_rcv.at[0], core_mate).wait_send()
    h_diag().wait_send()
    occ_out.wait()
    prep_out.wait()
    for size, sem in ((last, 2), (wide - last, 3)):
        cut = pl.ds(0, 4 * size)
        pltpu.make_async_copy(h_all.at[:, cut], h_hbm.at[:, cut], out_sem.at[sem]).wait()


def attend(x, ids_t, probs, w_q, w_k, w_v, w_o, group):
    tok, width = x.shape
    seq = tok * group
    kv_w = w_k.shape[1] // group
    kv_dev = kv_w // HEAD_DIM
    wide = w_q.shape[1] // group // kv_dev
    steps = width // wide
    dma = pltpu.SemaphoreType.DMA
    parts = len(PARTS)
    assert steps == 4 and kv_dev == 2 and group == 4
    return pl.pallas_call(
        attend_kernel,
        out_shape=(jax.ShapeDtypeStruct((seq, width), BF16), jax.ShapeDtypeStruct((1, HEAD_DIM), jnp.int32),
                   jax.ShapeDtypeStruct((8, seq), F32)),
        in_specs=[ANY] * 7,
        out_specs=(ANY, ANY, ANY),
        scratch_shapes=[
            pltpu.VMEM((SLOTS * wide, wide), BF16),
            pltpu.VMEM((width, 2 * kv_w), BF16),
            pltpu.VMEM((seq, width), BF16),
            pltpu.VMEM((seq, 2 * group * wide), BF16),
            pltpu.VMEM((seq, HEAD_DIM), F32),
            pltpu.VMEM((seq, width), BF16),
            pltpu.VMEM((seq, wide), F32),
            pltpu.VMEM((seq, 2 * kv_w), F32),
            pltpu.VMEM((seq, wide), BF16),
            pltpu.VMEM((seq, 2 * kv_w), BF16),
            pltpu.VMEM(x.shape, BF16), pltpu.VMEM(ids_t.shape, jnp.int32), pltpu.VMEM(probs.shape, F32),
            pltpu.VMEM((1, HEAD_DIM), jnp.int32), pltpu.VMEM((8, seq), F32),
            dma((8,)), dma((steps,)), dma((3 * parts + 1,)), dma((3,)), dma((4,)),
        ] + [dma, dma((steps,))] * 3 + [dma, dma((3,))] * 3 + [dma, dma((parts,))] * 3 + [dma, dma, dma((3,))],
        compiler_params=pltpu.CompilerParams(
            collective_id=0, has_side_effects=True, vmem_limit_bytes=66_000_000),
        cost_estimate=pl.CostEstimate(flops=seq * 2 * width * wide * 4, bytes_accessed=82_000_000, transcendentals=0),
        name='attend',
    )(x, ids_t, probs, w_q, w_k, w_v, w_o)


def dispatch_kernel(occ_hbm, prep_hbm, h_hbm, buf_hbm, out_hbm, occ_ref, h, prep_ref, zero, stage, todo,
                    e_sem, z_sem, p_sem, io_sem):
    me = lax.axis_index('sp')
    experts, seq, _ = buf_hbm.shape
    tok = out_hbm.shape[0]
    occ_copy = pltpu.make_async_copy(occ_hbm, occ_ref, io_sem.at[0])
    h_copy = pltpu.make_async_copy(h_hbm, h, io_sem.at[1])
    prep_copy = pltpu.make_async_copy(prep_hbm, prep_ref, io_sem.at[2])
    out_copy = pltpu.make_async_copy(h.at[span(me * tok, tok)], out_hbm, io_sem.at[3])
    occ_copy.start()
    h_copy.start()
    prep_copy.start()
    zero[...] = jnp.zeros_like(zero)
    for e in range(EARLY):
        pltpu.make_async_copy(zero, buf_hbm.at[e], e_sem).start()
    occ_copy.wait()

    def listed(e, count):
        used = occ_ref[0, e]

        @pl.when(used != 0)
        def _():
            todo[count] = e
        return count + used

    def filled(e, count):
        @pl.when(occ_ref[0, e] == 0)
        def _():
            pltpu.make_async_copy(zero, buf_hbm.at[e], z_sem).start()
        return listed(e, count)

    count = lax.fori_loop(0, EARLY, listed, 0)
    count = lax.fori_loop(EARLY, experts, filled, count)
    prep_copy.wait()
    h_copy.wait()
    out_copy.start()
    pltpu.make_async_copy(stage.at[pl.ds(0, EARLY)], buf_hbm.at[pl.ds(0, EARLY)], e_sem).wait()
    row = lax.broadcasted_iota(jnp.int32, (2 * seq, 1), 0)

    def batch_step(batch, carry):
        at = batch * 2
        key = jnp.where(row < seq, todo[at], todo[at + 1])
        key = ((key + me * experts) * seq + lax.rem(row, seq)).astype(F32)
        hit0 = key == prep_ref[0:1, :]
        hit1 = key == prep_ref[1:2, :]
        gate = jnp.sum(jnp.where(hit0, prep_ref[2:3, :], 0.0) + jnp.where(hit1, prep_ref[3:4, :], 0.0),
                       axis=1, keepdims=True)
        pick = jnp.where(hit0 | hit1, 1.0, 0.0).astype(BF16)
        rows = (gate * dot(pick, h[...])).astype(BF16)
        for i in range(2):
            stage[at + i] = rows[i * seq:(i + 1) * seq]
        for i in range(2):
            e = todo[at + i]

            @pl.when((at + i < count) & (e < EARLY))
            def _():
                pltpu.make_async_copy(stage.at[at + i], buf_hbm.at[e], p_sem.at[e]).start()

            @pl.when((at + i < count) & (e >= EARLY))
            def _():
                pltpu.make_async_copy(stage.at[at + i], buf_hbm.at[e], z_sem).start()
        return carry

    lax.fori_loop(0, (count + 1) // 2, batch_step, 0)
    for e in range(EARLY):
        @pl.when(occ_ref[0, e] != 0)
        def _():
            pltpu.make_async_copy(zero, buf_hbm.at[e], p_sem.at[e]).wait()
    rest = pl.ds(EARLY, experts - EARLY)
    pltpu.make_async_copy(stage.at[rest], buf_hbm.at[rest], z_sem).wait()
    out_copy.wait()


def dispatch(occ, prep, h, experts, tok):
    seq, width = h.shape
    dma = pltpu.SemaphoreType.DMA
    return pl.pallas_call(
        dispatch_kernel,
        out_shape=(jax.ShapeDtypeStruct((experts, seq, width), BF16), jax.ShapeDtypeStruct((tok, width), BF16)),
        in_specs=[ANY, ANY, ANY],
        out_specs=(ANY, ANY),
        scratch_shapes=[pltpu.SMEM((1, HEAD_DIM), jnp.int32), pltpu.VMEM((seq, width), BF16), pltpu.VMEM((8, seq), F32),
                        pltpu.VMEM((seq, width), BF16), pltpu.VMEM((experts, seq, width), BF16),
                        pltpu.SMEM((experts + 2,), jnp.int32), dma, dma, dma((EARLY,)), dma((4,))],
        compiler_params=pltpu.CompilerParams(vmem_limit_bytes=66_000_000),
        cost_estimate=pl.CostEstimate(flops=8_000_000_000, bytes_accessed=experts * seq * width * 2, transcendentals=0),
        name='dispatch',
    )(occ, prep, h)


def solution(mesh):
    group = mesh.shape['sp']
    row_spec = P(('dp', 'sp'), None)
    buf_spec = P(('dp', 'sp'), None, None)

    def device_step(x_loc, w_q, w_k, w_v, w_o, ids_loc, probs_loc):
        h, occ, prep = attend(x_loc, ids_loc.T, probs_loc, w_q, w_k, w_v, w_o, group)
        buf, hidden_out = dispatch(occ, prep, h, probs_loc.shape[1] // group, x_loc.shape[0])
        return hidden_out, buf

    return jax.shard_map(device_step, mesh=mesh, in_specs=(row_spec, P(), P(), P(), P(), row_spec, row_spec), out_specs=(row_spec, buf_spec), check_vma=False)
```

```python
import math
import jax
import jax.numpy as jnp
from jax import lax
from jax.experimental import pallas as pl
from jax.experimental.pallas import tpu as pltpu
from jax.sharding import PartitionSpec as P

HEAD_DIM = 128
SCORE_SCALE = 1.0 / math.sqrt(HEAD_DIM)
SLOTS = 10
PARTS = ((0, 512), (512, 512), (1024, 512))
HEAD = 512
SEGS = ((0, 1536), (0, 1024), (1024, 512))
EARLY = 4
ZERO_FIRST = 30
BLOCKS = 8
OCC = 256
PLACE = (8, 9, 0, 1, 2, 3, 4, 5)
MESH = pl.DeviceIdType.MESH
ANY = pl.BlockSpec(memory_space=pl.ANY)
VMEM = pl.BlockSpec(memory_space=pltpu.VMEM)
SMEM = pl.BlockSpec(memory_space=pltpu.SMEM)
F32, BF16 = jnp.float32, jnp.bfloat16


def peer_of(me, mask):
    chip = lax.rem(me // 2 + mask // 2, 2)
    core = lax.rem(lax.rem(me, 2) + mask % 2, 2)
    return chip * 2 + core


def span(start, size):
    return pl.ds(pl.multiple_of(start, size), size)


def dot(a, b):
    return jnp.dot(a, b, preferred_element_type=F32)


def attend_kernel(x_hbm, ids_hbm, probs_hbm, wq_hbm, wk_hbm, wv_hbm, wo_hbm, head_hbm, tail_hbm, occ_hbm, prep_hbm,
                  ring, kv_buf, x_all, o_all, m_all, h_all, acc, kv_acc, q_ref, kv_ref, x_ref, ids_ref, probs_ref,
                  occ_ref, prep_ref, w_sem, p_sem, in_sem, out_sem, x_snd, xs_rcv, xd_rcv, os_rcv, od_rcv, of_rcv,
                  hs_rcv, hd_rcv, hf_rcv, m_snd, m_rcv):
    me = lax.axis_index('sp')
    tok, width = x_ref.shape
    seq = x_all.shape[0]
    wide = ring.shape[1]
    steps = width // wide
    kv_w = kv_buf.shape[1] // 2
    heads = wide // HEAD_DIM
    experts = probs_ref.shape[1] // 4
    core_mate = peer_of(me, 1)
    chip_mate = peer_of(me, 2)
    mine = span(me * tok, tok)
    theirs = span(chip_mate * tok, tok)

    def q_copy(c):
        rows = span(c * wide, wide)
        return pltpu.make_async_copy(wq_hbm.at[rows, span(me * 2 * wide, wide)], ring.at[rows], w_sem.at[c])

    def r_copy(seg, c):
        off, size = SEGS[seg]
        cols = pl.ds(pl.multiple_of((me * 2 + 1) * wide + off, 512), size)
        return pltpu.make_async_copy(wq_hbm.at[span(c * wide, wide), cols],
                                     ring.at[span((c + 4) * wide, wide), pl.ds(off, size)], w_sem.at[2 + 2 * seg + c // 2])

    def r_dot(seg, half):
        off, size = SEGS[seg]
        deep = 2 * wide
        base = 4 * wide + half * deep
        pltpu.make_async_copy(wq_hbm.at[pl.ds(0, deep), pl.ds(0, size)], ring.at[pl.ds(base, deep), pl.ds(off, size)],
                              w_sem.at[2 + 2 * seg + half]).wait()
        return dot(x_all[:, half * deep:(half + 1) * deep], ring[base:base + deep, off:off + size])

    def k_copy(c):
        rows = span(c * wide, wide)
        return pltpu.make_async_copy(wk_hbm.at[rows, span(me * kv_w, kv_w)], kv_buf.at[rows, pl.ds(0, kv_w)], w_sem.at[c])

    def v_copy(c):
        rows = span(c * wide, wide)
        return pltpu.make_async_copy(wv_hbm.at[rows, span(me * kv_w, kv_w)], kv_buf.at[rows, pl.ds(kv_w, kv_w)], w_sem.at[c])

    def p_sem_at(p, i):
        return i // 2 if p == 0 else 4 + (i + 2) // 4 if p == 1 else 7 + (i + 2) // 4 + i // 7

    def p_copy(p, i):
        off, size = PARTS[p]
        return pltpu.make_async_copy(
            wo_hbm.at[span((peer_of(me, i % 4) * 2 + i // 4) * wide, wide), pl.ds(pl.multiple_of(me * wide + off, 128), size)],
            ring.at[pl.ds(PLACE[i] * wide, wide), pl.ds(off, size)], p_sem.at[p_sem_at(p, i)])

    def p_dot(p, i, count):
        off, size = PARTS[p]
        tile = ring.at[pl.ds(PLACE[i] * wide, count * wide), pl.ds(off, size)]
        pltpu.make_async_copy(wo_hbm.at[pl.ds(0, count * wide), pl.ds(0, size)], tile, p_sem.at[p_sem_at(p, i)]).wait()
        base = PLACE[i] * wide
        part = dot(o_all[:, i * wide:(i + count) * wide], ring[base:base + count * wide, off:off + size])
        if i == 0:
            acc[:, off:off + size] = part
        else:
            acc[:, off:off + size] += part

    def remote(src, dst, snd, rcv, to):
        return pltpu.make_async_remote_copy(src_ref=src, dst_ref=dst, send_sem=snd, recv_sem=rcv,
                                            device_id={'sp': to}, device_id_type=MESH)

    def x_far(c):
        cols = pl.ds(c * wide, wide)
        return remote(x_ref.at[:, cols], x_all.at[mine, cols], x_snd, xs_rcv.at[c], chip_mate)

    def x_near(c):
        cols = pl.ds(c * wide, wide)
        return remote(x_ref.at[:, cols], x_all.at[mine, cols], x_snd, xd_rcv.at[c], core_mate)

    def x_pass(c):
        cols = pl.ds(c * wide, wide)
        return remote(x_all.at[theirs, cols], x_all.at[theirs, cols], x_snd, xd_rcv.at[c], core_mate)

    def o_part(seg, r):
        off, size = SEGS[seg]
        return o_all.at[:, pl.ds((min(seg, 1) * 4 + r) * wide + off, size)]

    def o_far(seg):
        return remote(o_part(seg, 0), o_part(seg, 2), x_snd, os_rcv.at[seg], chip_mate)

    def o_near(seg):
        return remote(o_part(seg, 0), o_part(seg, 1), x_snd, od_rcv.at[seg], core_mate)

    def o_pass(seg):
        return remote(o_part(seg, 2), o_part(seg, 3), x_snd, of_rcv.at[seg], core_mate)

    def h_part(p, dev):
        off, size = PARTS[p]
        return h_all.at[:, pl.ds(pl.multiple_of(dev * wide + off, 128), size)]

    def h_far(p):
        return remote(h_part(p, me), h_part(p, me), x_snd, hs_rcv, chip_mate)

    def h_near(p):
        return remote(h_part(p, me), h_part(p, me), x_snd, hd_rcv, core_mate)

    def h_pass(p):
        return remote(h_part(p, chip_mate), h_part(p, chip_mate), x_snd, hf_rcv, core_mate)

    def m_send(mask):
        return remote(m_all.at[mine], m_all.at[mine], m_snd, m_rcv, peer_of(me, mask))

    barrier = pltpu.get_barrier_semaphore()
    for mask in (1, 2, 3):
        pl.semaphore_signal(barrier, inc=1, device_id={'sp': peer_of(me, mask)}, device_id_type=MESH)
    x_in = pltpu.make_async_copy(x_hbm, x_ref, in_sem.at[0])
    ids_in = pltpu.make_async_copy(ids_hbm, ids_ref, in_sem.at[1])
    probs_in = pltpu.make_async_copy(probs_hbm, probs_ref, in_sem.at[2])
    x_in.start()
    ids_in.start()
    probs_in.start()

    def start_first(c, carry):
        q_copy(c).start()
        k_copy(c).start()
        v_copy(c).start()
        return carry

    def start_second(c, carry):
        r_copy(1, c).start()
        return carry

    def start_third(c, carry):
        r_copy(2, c).start()
        return carry

    lax.fori_loop(0, 4, start_first, 0)
    lax.fori_loop(0, 4, start_second, 0)
    lax.fori_loop(0, 4, start_third, 0)
    p_copy(0, 0).start()
    p_copy(0, 1).start()
    x_in.wait()
    pl.semaphore_wait(barrier, 3)
    for c in range(steps):
        x_far(c).start()
        x_near(c).start()
    x_all[mine, :] = x_ref[...]
    ids_in.wait()
    probs_in.wait()
    ids = ids_ref[...].astype(F32)
    probs = probs_ref[...]
    eye = lax.broadcasted_iota(jnp.int32, (tok, tok), 0) == lax.broadcasted_iota(jnp.int32, (tok, tok), 1)
    id0 = jnp.sum(jnp.where(eye, ids[0:1, :], 0.0), axis=1, keepdims=True)
    id1 = jnp.sum(jnp.where(eye, ids[1:2, :], 0.0), axis=1, keepdims=True)
    lanes = lax.broadcasted_iota(jnp.int32, probs.shape, 1).astype(F32)
    p0 = jnp.sum(jnp.where(lanes == id0, probs, 0.0), axis=1, keepdims=True)
    p1 = jnp.sum(jnp.where(lanes == id1, probs, 0.0), axis=1, keepdims=True)
    total = p0 + p1
    cols = lax.broadcasted_iota(jnp.int32, (tok, HEAD_DIM), 1)
    m_all[mine, :] = jnp.where(cols == 0, id0, jnp.where(cols == 1, id1,
                     jnp.where(cols == 2, p0 / total, jnp.where(cols == 3, p1 / total, 0.0))))
    for mask in (1, 2, 3):
        m_send(mask).start()
    def first_dots(c):
        pair = x_all.at[pl.ds(0, 2 * tok), pl.ds(c * wide, wide)]
        remote(pair, pair, x_snd, xd_rcv.at[c], core_mate).wait_recv()
        chunk = pl.ds(0, wide + 2 * kv_w)
        pltpu.make_async_copy(wq_hbm.at[chunk, pl.ds(0, wide)], ring.at[chunk], w_sem.at[c]).wait()
        x = x_all[:, c * wide:(c + 1) * wide]
        part = dot(x, kv_buf[c * wide:(c + 1) * wide, :])
        if c == 0:
            kv_acc[...] = part
        else:
            kv_acc[...] += part
        part = dot(x, ring[c * wide:(c + 1) * wide, :])
        if c == 0:
            acc[...] = part
        else:
            acc[...] += part

    for c in range(steps):
        x_far(c).wait_recv()
        x_pass(c).start()
        if c > 0:
            first_dots(c - 1)
    first_dots(steps - 1)

    def attention(seg):
        kv = min(seg, 1)
        start, size = SEGS[seg]
        heads = size // HEAD_DIM
        k = kv_ref[:, kv * HEAD_DIM:(kv + 1) * HEAD_DIM]
        v = kv_ref[:, kv_w + kv * HEAD_DIM:kv_w + (kv + 1) * HEAD_DIM]
        cuts = [slice(start + m * HEAD_DIM, start + (m + 1) * HEAD_DIM) for m in range(heads)]
        q = jnp.concatenate([q_ref[:, c] for c in cuts], axis=0)
        s = lax.dot_general(q, k, (((1,), (1,)), ((), ())), preferred_element_type=F32) * SCORE_SCALE
        row = lax.rem(lax.broadcasted_iota(jnp.int32, s.shape, 0), seq)
        s = jnp.where(row >= lax.broadcasted_iota(jnp.int32, s.shape, 1), s, -1e30)
        e = jnp.exp(s - jnp.max(s, axis=1, keepdims=True))
        w = (e / jnp.sum(e, axis=1, keepdims=True)).astype(BF16)
        o = dot(w, v).astype(BF16)
        for m, c in enumerate(cuts):
            o_all[:, kv * 4 * wide + c.start:kv * 4 * wide + c.stop] = o[m * seq:(m + 1) * seq]
        o_far(seg).start()
        o_near(seg).start()

    kv_ref[...] = kv_acc[...].astype(BF16)
    q_ref[...] = acc[...].astype(BF16)
    for i in (2, 3, 4, 5):
        p_copy(0, i).start()
    attention(0)

    mid = SEGS[2][0]
    acc[:, :mid] = r_dot(1, 0)
    q_ref[:, :mid] = (acc[:, :mid] + r_dot(1, 1)).astype(BF16)
    attention(1)
    acc[:, mid:] = r_dot(2, 0)
    p_copy(0, 6).start()
    p_copy(0, 7).start()
    q_ref[:, mid:] = (acc[:, mid:] + r_dot(2, 1)).astype(BF16)
    for i in range(8):
        p_copy(1, i).start()
    attention(2)

    def routing():
        remote(m_all.at[pl.ds(0, 3 * tok)], m_all.at[pl.ds(0, 3 * tok)], m_snd, m_rcv, core_mate).wait_recv()
        meta = m_all[...]
        rows = meta.T
        t_col = lax.broadcasted_iota(jnp.int32, (seq, seq), 0)
        t_row = lax.broadcasted_iota(jnp.int32, (seq, seq), 1)
        before = (t_col < t_row) & (t_col // tok == t_row // tok)
        source = (lax.broadcasted_iota(jnp.int32, (1, seq), 1) // tok).astype(F32)
        for k in range(2):
            same = (meta[:, 0:1] == rows[k:k + 1, :]) | (meta[:, 1:2] == rows[k:k + 1, :])
            rank = jnp.sum(jnp.where(before & same, 1.0, 0.0), axis=0, keepdims=True)
            prep_ref[k:k + 1, :] = (rows[k:k + 1, :] * 4.0 + source) * tok + rank
        prep_ref[2:4, :] = rows[2:4, :]
        prep_ref[4:8, :] = jnp.zeros((4, seq), F32)
        block = (lax.broadcasted_iota(jnp.int32, (seq, OCC), 1) + me * experts * 4).astype(F32)
        origin = (lax.broadcasted_iota(jnp.int32, (seq, 1), 0) // tok).astype(F32)
        used = (meta[:, 0:1] * 4.0 + origin == block) | (meta[:, 1:2] * 4.0 + origin == block)
        occ_ref[...] = jnp.max(jnp.where(used, 1, 0), axis=0, keepdims=True)
        occ_out = pltpu.make_async_copy(occ_ref, occ_hbm, out_sem.at[0])
        prep_out = pltpu.make_async_copy(prep_ref, prep_hbm, out_sem.at[1])
        occ_out.start()
        prep_out.start()
        return occ_out, prep_out

    def finish(p):
        off, size = PARTS[p]
        home = pl.ds(pl.multiple_of(me * wide + off, 512), size)
        h_all[:, home] = (x_all[:, home].astype(F32) + acc[:, off:off + size]).astype(BF16)
        if p == 0:
            h_far(0).start()
        h_near(p).start()

    o_near(0).wait_recv()
    p_dot(0, 0, 2)
    for i in range(8):
        p_copy(2, i).start()
    occ_out, prep_out = routing()
    o_far(0).wait_recv()
    o_pass(0).start()
    o_near(1).wait_recv()
    o_near(2).wait_recv()
    p_dot(0, 4, 2)
    o_pass(0).wait_recv()
    p_dot(0, 2, 2)
    p_dot(1, 0, 2)
    o_far(1).wait_recv()
    o_pass(1).start()
    p_dot(1, 2, 4)
    o_far(2).wait_recv()
    o_pass(2).start()
    o_pass(1).wait_recv()
    o_pass(2).wait_recv()
    p_dot(0, 6, 2)
    finish(0)
    p_dot(1, 6, 2)
    finish(1)
    p_dot(2, 0, 2)
    p_dot(2, 2, 4)
    p_dot(2, 6, 1)
    p_dot(2, 7, 1)
    finish(2)

    h_far(0).wait_recv()
    h_pass(0).start()
    whole = h_all.at[:, pl.ds(0, wide)]
    remote(whole, whole, x_snd, hd_rcv, core_mate).wait_recv()
    for core in range(2):
        rest = wide - HEAD
        cut = pl.ds(pl.multiple_of((me // 2 * 2 + core) * wide + HEAD, 512), rest)
        pltpu.make_async_copy(h_all.at[:, cut], tail_hbm.at[:, pl.ds(core * rest, rest)], out_sem.at[3]).start()
    h_pass(0).wait_recv()
    for dev in range(4):
        pltpu.make_async_copy(h_all.at[:, pl.ds(dev * wide, HEAD)], head_hbm.at[:, pl.ds(dev * HEAD, HEAD)],
                              out_sem.at[2]).start()

    remote(m_all.at[pl.ds(0, 3 * tok)], m_all.at[pl.ds(0, 3 * tok)], m_snd, m_rcv, core_mate).wait_send()
    sent = (3 * tok * width + 6 * seq * wide + seq * wide + 2 * seq * HEAD) // 1024
    sends = ring.at[pl.ds(0, sent), pl.ds(0, 1024)]
    remote(sends, sends, x_snd, hs_rcv, core_mate).wait_send()
    occ_out.wait()
    prep_out.wait()
    pltpu.make_async_copy(h_all.at[:, pl.ds(0, 2 * (wide - HEAD))], tail_hbm, out_sem.at[3]).wait()
    pltpu.make_async_copy(h_all.at[:, pl.ds(0, 4 * HEAD)], head_hbm, out_sem.at[2]).wait()


def attend(x, ids_t, probs, w_q, w_k, w_v, w_o, group):
    tok, width = x.shape
    seq = tok * group
    kv_w = w_k.shape[1] // group
    kv_dev = kv_w // HEAD_DIM
    wide = w_q.shape[1] // group // kv_dev
    steps = width // wide
    dma = pltpu.SemaphoreType.DMA
    parts = len(PARTS)
    assert steps == 4 and kv_dev == 2 and group == 4
    return pl.pallas_call(
        attend_kernel,
        out_shape=(jax.ShapeDtypeStruct((seq, 4 * HEAD), BF16), jax.ShapeDtypeStruct((seq, 2 * (wide - HEAD)), BF16),
                   jax.ShapeDtypeStruct((1, OCC), jnp.int32),
                   jax.ShapeDtypeStruct((8, seq), F32)),
        in_specs=[ANY] * 7,
        out_specs=(ANY, ANY, ANY, ANY),
        scratch_shapes=[
            pltpu.VMEM((SLOTS * wide, wide), BF16),
            pltpu.VMEM((width, 2 * kv_w), BF16),
            pltpu.VMEM((seq, width), BF16),
            pltpu.VMEM((seq, 2 * group * wide), BF16),
            pltpu.VMEM((seq, HEAD_DIM), F32),
            pltpu.VMEM((seq, width), BF16),
            pltpu.VMEM((seq, wide), F32),
            pltpu.VMEM((seq, 2 * kv_w), F32),
            pltpu.VMEM((seq, wide), BF16),
            pltpu.VMEM((seq, 2 * kv_w), BF16),
            pltpu.VMEM(x.shape, BF16), pltpu.VMEM(ids_t.shape, jnp.int32), pltpu.VMEM(probs.shape, F32),
            pltpu.VMEM((1, OCC), jnp.int32), pltpu.VMEM((8, seq), F32),
            dma((8,)), dma((11,)), dma((3,)), dma((4,)),
            dma, dma((steps,)), dma((steps,)), dma((3,)), dma((3,)), dma((3,)), dma, dma, dma, dma, dma],
        compiler_params=pltpu.CompilerParams(
            collective_id=0, has_side_effects=True, vmem_limit_bytes=66_000_000),
        cost_estimate=pl.CostEstimate(flops=seq * 2 * width * wide * 4, bytes_accessed=82_000_000, transcendentals=0),
        name='attend',
    )(x, ids_t, probs, w_q, w_k, w_v, w_o)


def zero_kernel(occ_hbm, buf_hbm, list_hbm, occ_ref, list_ref, zero, z_sem, io_sem):
    experts = buf_hbm.shape[0]
    occ_copy = pltpu.make_async_copy(occ_hbm, occ_ref, io_sem.at[0])
    list_copy = pltpu.make_async_copy(list_ref, list_hbm, io_sem.at[1])
    occ_copy.start()
    zero[...] = jnp.zeros_like(zero)
    lax.fori_loop(0, ZERO_FIRST, lambda e, c: (pltpu.make_async_copy(zero, buf_hbm.at[e], z_sem).start(), c)[1], 0)
    occ_copy.wait()

    def expert(e, count):
        for i in range(4):
            one = occ_ref[0, e * 4 + i]

            @pl.when(one != 0)
            def _():
                list_ref[0, count] = e * 4 + i
            count = count + one
        return count

    list_ref[0, OCC - 1] = lax.fori_loop(0, experts, expert, 0)
    list_copy.start()
    filled = buf_hbm.at[pl.ds(0, ZERO_FIRST)]
    pltpu.make_async_copy(filled, filled, z_sem).wait()
    list_copy.wait()


def zero_most(occ, experts, seq, width):
    dma = pltpu.SemaphoreType.DMA
    return pl.pallas_call(
        zero_kernel,
        out_shape=(jax.ShapeDtypeStruct((experts, seq, width), BF16), jax.ShapeDtypeStruct((1, OCC), jnp.int32)),
        in_specs=[ANY],
        out_specs=(ANY, ANY),
        scratch_shapes=[pltpu.SMEM((1, OCC), jnp.int32), pltpu.SMEM((1, OCC), jnp.int32), pltpu.VMEM((seq, width), BF16),
                        dma, dma((2,))],
        compiler_params=pltpu.CompilerParams(vmem_limit_bytes=67_043_328),
        cost_estimate=pl.CostEstimate(flops=8_000_000_000, bytes_accessed=ZERO_FIRST * seq * width * 2, transcendentals=0),
        name='zero_most',
    )(occ)


def dispatch_kernel(list_hbm, occ_hbm, prep_hbm, head_hbm, tail_hbm, far_hbm, buf_in, buf_hbm, out_hbm, list_ref, occ_ref,
                    h, prep_ref, zero, stage, e_sem, z_sem, p_sem, io_sem, h_sem):
    me = lax.axis_index('sp')
    experts, seq, width = buf_hbm.shape
    tok = out_hbm.shape[0]
    wide = width // 4
    rest = wide - HEAD
    settled = ZERO_FIRST + EARLY
    list_copy = pltpu.make_async_copy(list_hbm, list_ref, io_sem.at[0])
    occ_copy = pltpu.make_async_copy(occ_hbm, occ_ref, io_sem.at[1])
    prep_copy = pltpu.make_async_copy(prep_hbm, prep_ref, io_sem.at[2])
    out_copy = pltpu.make_async_copy(h.at[span(me * tok, tok)], out_hbm, io_sem.at[3])
    list_copy.start()
    occ_copy.start()
    prep_copy.start()
    for dev in range(4):
        pltpu.make_async_copy(head_hbm.at[:, pl.ds(dev * HEAD, HEAD)], h.at[:, pl.ds(dev * wide, HEAD)], h_sem).start()
    for chip, src in ((me // 2, tail_hbm), (1 - me // 2, far_hbm)):
        for core in range(2):
            cut = pl.ds(pl.multiple_of((chip * 2 + core) * wide + HEAD, 512), rest)
            pltpu.make_async_copy(src.at[:, pl.ds(core * rest, rest)], h.at[:, cut], h_sem).start()
    zero[...] = jnp.zeros_like(zero)
    for e in range(ZERO_FIRST, settled):
        pltpu.make_async_copy(zero, buf_hbm.at[e], e_sem).start()
    list_copy.wait()
    occ_copy.wait()

    def place(b):
        return buf_hbm.at[b // 4, span(lax.rem(b, 4) * tok, tok)]

    def fill(e, carry):
        ones = [occ_ref[0, e * 4 + i] for i in range(4)]
        used = ones[0] + ones[1] + ones[2] + ones[3]

        @pl.when(used == 0)
        def _():
            pltpu.make_async_copy(zero, buf_hbm.at[e], z_sem).start()

        @pl.when(used != 0)
        def _():
            for i in range(4):
                @pl.when(ones[i] == 0)
                def _():
                    pltpu.make_async_copy(zero.at[pl.ds(0, tok)], place(e * 4 + i), z_sem).start()
        return carry

    lax.fori_loop(settled, experts, fill, 0)
    count = list_ref[0, OCC - 1]
    prep_copy.wait()
    pltpu.make_async_copy(buf_hbm.at[0], h, h_sem).wait()
    out_copy.start()
    row = lax.broadcasted_iota(jnp.int32, (BLOCKS * tok, 1), 0)

    def batch_step(batch, carry):
        at = batch * BLOCKS
        key = jnp.zeros((BLOCKS * tok, 1), jnp.int32)
        for i in range(BLOCKS):
            key = jnp.where(row // tok == i, list_ref[0, at + i], key)
        key = ((key + me * experts * 4) * tok + lax.rem(row, tok)).astype(F32)
        hit0 = key == prep_ref[0:1, :]
        hit1 = key == prep_ref[1:2, :]
        gate = jnp.sum(jnp.where(hit0, prep_ref[2:3, :], 0.0) + jnp.where(hit1, prep_ref[3:4, :], 0.0),
                       axis=1, keepdims=True)
        pick = jnp.where(hit0 | hit1, 1.0, 0.0).astype(BF16)
        rows = (gate * dot(pick, h[...])).astype(BF16)
        for i in range(BLOCKS):
            stage[at + i] = rows[i * tok:(i + 1) * tok]

        @pl.when(batch == 0)
        def _():
            early = buf_hbm.at[pl.ds(ZERO_FIRST, EARLY)]
            pltpu.make_async_copy(early, early, e_sem).wait()

        for i in range(BLOCKS):
            b = list_ref[0, at + i]

            @pl.when((at + i < count) & (b < settled * 4))
            def _():
                pltpu.make_async_copy(stage.at[at + i], place(b), p_sem).start()

            @pl.when((at + i < count) & (b >= settled * 4))
            def _():
                pltpu.make_async_copy(stage.at[at + i], place(b), z_sem).start()
        return carry

    lax.fori_loop(0, jnp.maximum((count + BLOCKS - 1) // BLOCKS, 1), batch_step, 0)

    def landed(i, carry):
        @pl.when(list_ref[0, i] < settled * 4)
        def _():
            pltpu.make_async_copy(stage.at[0], place(0), p_sem).wait()
        return carry

    lax.fori_loop(0, count, landed, 0)
    others = buf_hbm.at[pl.ds(settled, experts - settled)]
    pltpu.make_async_copy(others, others, z_sem).wait()
    out_copy.wait()


def dispatch(blocks, occ, prep, head, tail, far, buf, tok):
    experts, seq, width = buf.shape
    dma = pltpu.SemaphoreType.DMA
    return pl.pallas_call(
        dispatch_kernel,
        out_shape=(jax.ShapeDtypeStruct(buf.shape, BF16), jax.ShapeDtypeStruct((tok, width), BF16)),
        in_specs=[ANY] * 7,
        out_specs=(ANY, ANY),
        input_output_aliases={6: 0},
        scratch_shapes=[pltpu.SMEM((1, OCC), jnp.int32), pltpu.SMEM((1, OCC), jnp.int32),
                        pltpu.VMEM((seq, width), BF16), pltpu.VMEM((8, seq), F32), pltpu.VMEM((seq, width), BF16),
                        pltpu.VMEM((experts * 4, tok, width), BF16), dma, dma, dma, dma((4,)), dma],
        compiler_params=pltpu.CompilerParams(vmem_limit_bytes=66_000_000),
        cost_estimate=pl.CostEstimate(flops=4_000_000_000, bytes_accessed=experts * seq * width, transcendentals=0),
        name='dispatch',
    )(blocks, occ, prep, head, tail, far, buf)


def solution(mesh):
    group = mesh.shape['sp']
    row_spec = P(('dp', 'sp'), None)
    buf_spec = P(('dp', 'sp'), None, None)

    def device_step(x_loc, w_q, w_k, w_v, w_o, ids_loc, probs_loc):
        head, tail, occ, prep = attend(x_loc, ids_loc.T, probs_loc, w_q, w_k, w_v, w_o, group)
        far = lax.ppermute(tail, 'sp', [(i, (i + 2) % group) for i in range(group)])
        buf, blocks = zero_most(occ, probs_loc.shape[1] // group, head.shape[0], x_loc.shape[1])
        buf, hidden_out = dispatch(blocks, occ, prep, head, tail, far, buf, x_loc.shape[0])
        return hidden_out, buf

    return jax.shard_map(device_step, mesh=mesh, in_specs=(row_spec, P(), P(), P(), P(), row_spec, row_spec), out_specs=(row_spec, buf_spec), check_vma=False)
```

```python
import math
import jax
import jax.numpy as jnp
from jax import lax
from jax.experimental import pallas as pl
from jax.experimental.pallas import tpu as pltpu
from jax.sharding import PartitionSpec as P

HEAD_DIM = 128
SCORE_SCALE = 1.0 / math.sqrt(HEAD_DIM)
SLOTS = 10
PARTS = ((0, 512), (512, 512), (1024, 512))
HEAD = 512
SEGS = ((0, 1536), (0, 1024), (1024, 512))
EARLY = 3
ZERO_FIRST = 31
BLIND = 4
BLOCKS = 8
OCC = 256
PLACE = (8, 9, 0, 1, 2, 3, 4, 5)
MESH = pl.DeviceIdType.MESH
ANY = pl.BlockSpec(memory_space=pl.ANY)
VMEM = pl.BlockSpec(memory_space=pltpu.VMEM)
SMEM = pl.BlockSpec(memory_space=pltpu.SMEM)
F32, BF16 = jnp.float32, jnp.bfloat16


def peer_of(me, mask):
    chip = lax.rem(me // 2 + mask // 2, 2)
    core = lax.rem(lax.rem(me, 2) + mask % 2, 2)
    return chip * 2 + core


def span(start, size):
    return pl.ds(pl.multiple_of(start, size), size)


def dot(a, b):
    return jnp.dot(a, b, preferred_element_type=F32)


def attend_kernel(x_hbm, ids_hbm, probs_hbm, wq_hbm, wk_hbm, wv_hbm, wo_hbm, head_hbm, tail_hbm, occ_hbm, prep_hbm,
                  ring, kv_buf, x_all, o_all, m_all, h_all, acc, kv_acc, q_ref, kv_ref, x_ref, ids_ref, probs_ref,
                  occ_ref, prep_ref, w_sem, p_sem, in_sem, out_sem, x_snd, xs_rcv, xd_rcv, os_rcv, od_rcv, of_rcv,
                  hs_rcv, hd_rcv, hf_rcv, m_snd, m_rcv):
    me = lax.axis_index('sp')
    tok, width = x_ref.shape
    seq = x_all.shape[0]
    wide = ring.shape[1]
    steps = width // wide
    kv_w = kv_buf.shape[1] // 2
    heads = wide // HEAD_DIM
    experts = probs_ref.shape[1] // 4
    core_mate = peer_of(me, 1)
    chip_mate = peer_of(me, 2)
    mine = span(me * tok, tok)
    theirs = span(chip_mate * tok, tok)

    def q_copy(c):
        rows = span(c * wide, wide)
        return pltpu.make_async_copy(wq_hbm.at[rows, span(me * 2 * wide, wide)], ring.at[rows], w_sem.at[c])

    def r_copy(seg, c):
        off, size = SEGS[seg]
        cols = pl.ds(pl.multiple_of((me * 2 + 1) * wide + off, 512), size)
        return pltpu.make_async_copy(wq_hbm.at[span(c * wide, wide), cols],
                                     ring.at[span((c + 4) * wide, wide), pl.ds(off, size)], w_sem.at[2 + 2 * seg + c // 2])

    def r_dot(seg, half):
        off, size = SEGS[seg]
        deep = 2 * wide
        base = 4 * wide + half * deep
        pltpu.make_async_copy(wq_hbm.at[pl.ds(0, deep), pl.ds(0, size)], ring.at[pl.ds(base, deep), pl.ds(off, size)],
                              w_sem.at[2 + 2 * seg + half]).wait()
        return dot(x_all[:, half * deep:(half + 1) * deep], ring[base:base + deep, off:off + size])

    def k_copy(c):
        rows = span(c * wide, wide)
        return pltpu.make_async_copy(wk_hbm.at[rows, span(me * kv_w, kv_w)], kv_buf.at[rows, pl.ds(0, kv_w)], w_sem.at[c])

    def v_copy(c):
        rows = span(c * wide, wide)
        return pltpu.make_async_copy(wv_hbm.at[rows, span(me * kv_w, kv_w)], kv_buf.at[rows, pl.ds(kv_w, kv_w)], w_sem.at[c])

    def p_sem_at(p, i):
        return i // 2 if p == 0 else 4 + (i + 2) // 4 if p == 1 else 7 + (i + 2) // 4 + i // 7

    def p_copy(p, i):
        off, size = PARTS[p]
        return pltpu.make_async_copy(
            wo_hbm.at[span((peer_of(me, i % 4) * 2 + i // 4) * wide, wide), pl.ds(pl.multiple_of(me * wide + off, 128), size)],
            ring.at[pl.ds(PLACE[i] * wide, wide), pl.ds(off, size)], p_sem.at[p_sem_at(p, i)])

    def p_dot(p, i, count, waits=None):
        off, size = PARTS[p]
        waits = count if waits is None else waits
        if waits:
            tile = ring.at[pl.ds(PLACE[i] * wide, waits * wide), pl.ds(off, size)]
            pltpu.make_async_copy(wo_hbm.at[pl.ds(0, waits * wide), pl.ds(0, size)], tile, p_sem.at[p_sem_at(p, i)]).wait()
        base = PLACE[i] * wide
        part = dot(o_all[:, i * wide:(i + count) * wide], ring[base:base + count * wide, off:off + size])
        if i == 0:
            acc[:, off:off + size] = part
        else:
            acc[:, off:off + size] += part

    def remote(src, dst, snd, rcv, to):
        return pltpu.make_async_remote_copy(src_ref=src, dst_ref=dst, send_sem=snd, recv_sem=rcv,
                                            device_id={'sp': to}, device_id_type=MESH)

    def x_far(c):
        cols = pl.ds(c * wide, wide)
        return remote(x_ref.at[:, cols], x_all.at[mine, cols], x_snd, xs_rcv.at[c], chip_mate)

    def x_near(c):
        cols = pl.ds(c * wide, wide)
        return remote(x_ref.at[:, cols], x_all.at[mine, cols], x_snd, xd_rcv.at[c], core_mate)

    def x_pass(c):
        cols = pl.ds(c * wide, wide)
        return remote(x_all.at[theirs, cols], x_all.at[theirs, cols], x_snd, xd_rcv.at[c], core_mate)

    def o_part(seg, r):
        off, size = SEGS[seg]
        return o_all.at[:, pl.ds((min(seg, 1) * 4 + r) * wide + off, size)]

    def o_far(seg):
        return remote(o_part(seg, 0), o_part(seg, 2), x_snd, os_rcv.at[seg], chip_mate)

    def o_near(seg):
        return remote(o_part(seg, 0), o_part(seg, 1), x_snd, od_rcv.at[seg], core_mate)

    def o_pass(seg):
        return remote(o_part(seg, 2), o_part(seg, 3), x_snd, of_rcv.at[seg], core_mate)

    def h_part(p, dev):
        off, size = PARTS[p]
        return h_all.at[:, pl.ds(pl.multiple_of(dev * wide + off, 128), size)]

    def h_far(p):
        return remote(h_part(p, me), h_part(p, me), x_snd, hs_rcv, chip_mate)

    def h_near(p):
        return remote(h_part(p, me), h_part(p, me), x_snd, hd_rcv, core_mate)

    def h_pass(p):
        return remote(h_part(p, chip_mate), h_part(p, chip_mate), x_snd, hf_rcv, core_mate)

    def m_send(mask):
        return remote(m_all.at[mine], m_all.at[mine], m_snd, m_rcv, peer_of(me, mask))

    barrier = pltpu.get_barrier_semaphore()
    for mask in (1, 2, 3):
        pl.semaphore_signal(barrier, inc=1, device_id={'sp': peer_of(me, mask)}, device_id_type=MESH)
    x_in = pltpu.make_async_copy(x_hbm, x_ref, in_sem.at[0])
    ids_in = pltpu.make_async_copy(ids_hbm, ids_ref, in_sem.at[1])
    probs_in = pltpu.make_async_copy(probs_hbm, probs_ref, in_sem.at[2])
    x_in.start()
    ids_in.start()
    probs_in.start()

    def start_first(c, carry):
        q_copy(c).start()
        k_copy(c).start()
        v_copy(c).start()
        return carry

    def start_second(c, carry):
        r_copy(1, c).start()
        return carry

    def start_third(c, carry):
        r_copy(2, c).start()
        return carry

    lax.fori_loop(0, 4, start_first, 0)
    lax.fori_loop(0, 4, start_second, 0)
    lax.fori_loop(0, 4, start_third, 0)
    p_copy(0, 0).start()
    p_copy(0, 1).start()
    x_in.wait()
    pl.semaphore_wait(barrier, 3)
    for c in range(steps):
        x_far(c).start()
        x_near(c).start()
    x_all[mine, :] = x_ref[...]
    ids_in.wait()
    probs_in.wait()
    ids = ids_ref[...].astype(F32)
    probs = probs_ref[...]
    eye = lax.broadcasted_iota(jnp.int32, (tok, tok), 0) == lax.broadcasted_iota(jnp.int32, (tok, tok), 1)
    id0 = jnp.sum(jnp.where(eye, ids[0:1, :], 0.0), axis=1, keepdims=True)
    id1 = jnp.sum(jnp.where(eye, ids[1:2, :], 0.0), axis=1, keepdims=True)
    lanes = lax.broadcasted_iota(jnp.int32, probs.shape, 1).astype(F32)
    p0 = jnp.sum(jnp.where(lanes == id0, probs, 0.0), axis=1, keepdims=True)
    p1 = jnp.sum(jnp.where(lanes == id1, probs, 0.0), axis=1, keepdims=True)
    total = p0 + p1
    cols = lax.broadcasted_iota(jnp.int32, (tok, HEAD_DIM), 1)
    m_all[mine, :] = jnp.where(cols == 0, id0, jnp.where(cols == 1, id1,
                     jnp.where(cols == 2, p0 / total, jnp.where(cols == 3, p1 / total, 0.0))))
    for mask in (1, 2, 3):
        m_send(mask).start()
    def first_dots(c):
        pair = x_all.at[pl.ds(0, 2 * tok), pl.ds(c * wide, wide)]
        remote(pair, pair, x_snd, xd_rcv.at[c], core_mate).wait_recv()
        chunk = pl.ds(0, wide + 2 * kv_w)
        pltpu.make_async_copy(wq_hbm.at[chunk, pl.ds(0, wide)], ring.at[chunk], w_sem.at[c]).wait()
        x = x_all[:, c * wide:(c + 1) * wide]
        part = dot(x, kv_buf[c * wide:(c + 1) * wide, :])
        if c == 0:
            kv_acc[...] = part
        else:
            kv_acc[...] += part
        part = dot(x, ring[c * wide:(c + 1) * wide, :])
        if c == 0:
            acc[...] = part
        else:
            acc[...] += part

    for c in range(steps):
        x_far(c).wait_recv()
        x_pass(c).start()
        if c > 0:
            first_dots(c - 1)
    first_dots(steps - 1)

    def attention(seg):
        kv = min(seg, 1)
        start, size = SEGS[seg]
        heads = size // HEAD_DIM
        k = kv_ref[:, kv * HEAD_DIM:(kv + 1) * HEAD_DIM]
        v = kv_ref[:, kv_w + kv * HEAD_DIM:kv_w + (kv + 1) * HEAD_DIM]
        cuts = [slice(start + m * HEAD_DIM, start + (m + 1) * HEAD_DIM) for m in range(heads)]
        q = jnp.concatenate([q_ref[:, c] for c in cuts], axis=0)
        s = lax.dot_general(q, k, (((1,), (1,)), ((), ())), preferred_element_type=F32) * SCORE_SCALE
        row = lax.rem(lax.broadcasted_iota(jnp.int32, s.shape, 0), seq)
        s = jnp.where(row >= lax.broadcasted_iota(jnp.int32, s.shape, 1), s, -1e30)
        e = jnp.exp(s - jnp.max(s, axis=1, keepdims=True))
        w = (e / jnp.sum(e, axis=1, keepdims=True)).astype(BF16)
        o = dot(w, v).astype(BF16)
        for m, c in enumerate(cuts):
            o_all[:, kv * 4 * wide + c.start:kv * 4 * wide + c.stop] = o[m * seq:(m + 1) * seq]
        o_far(seg).start()
        o_near(seg).start()

    kv_ref[...] = kv_acc[...].astype(BF16)
    q_ref[...] = acc[...].astype(BF16)
    for i in (2, 3, 4, 5):
        p_copy(0, i).start()
    attention(0)

    mid = SEGS[2][0]
    acc[:, :mid] = r_dot(1, 0)
    q_ref[:, :mid] = (acc[:, :mid] + r_dot(1, 1)).astype(BF16)
    attention(1)
    acc[:, mid:] = r_dot(2, 0)
    p_copy(0, 6).start()
    p_copy(0, 7).start()
    q_ref[:, mid:] = (acc[:, mid:] + r_dot(2, 1)).astype(BF16)
    for i in range(8):
        p_copy(1, i).start()
    attention(2)

    def routing():
        remote(m_all.at[pl.ds(0, 3 * tok)], m_all.at[pl.ds(0, 3 * tok)], m_snd, m_rcv, core_mate).wait_recv()
        meta = m_all[...]
        rows = meta.T
        t_col = lax.broadcasted_iota(jnp.int32, (seq, seq), 0)
        t_row = lax.broadcasted_iota(jnp.int32, (seq, seq), 1)
        before = (t_col < t_row) & (t_col // tok == t_row // tok)
        source = (lax.broadcasted_iota(jnp.int32, (1, seq), 1) // tok).astype(F32)
        for k in range(2):
            same = (meta[:, 0:1] == rows[k:k + 1, :]) | (meta[:, 1:2] == rows[k:k + 1, :])
            rank = jnp.sum(jnp.where(before & same, 1.0, 0.0), axis=0, keepdims=True)
            prep_ref[k:k + 1, :] = (rows[k:k + 1, :] * 4.0 + source) * tok + rank
        prep_ref[2:4, :] = rows[2:4, :]
        prep_ref[4:8, :] = jnp.zeros((4, seq), F32)
        block = (lax.broadcasted_iota(jnp.int32, (seq, OCC), 1) + me * experts * 4).astype(F32)
        origin = (lax.broadcasted_iota(jnp.int32, (seq, 1), 0) // tok).astype(F32)
        used = (meta[:, 0:1] * 4.0 + origin == block) | (meta[:, 1:2] * 4.0 + origin == block)
        occ_ref[...] = jnp.max(jnp.where(used, 1, 0), axis=0, keepdims=True)
        occ_out = pltpu.make_async_copy(occ_ref, occ_hbm, out_sem.at[0])
        prep_out = pltpu.make_async_copy(prep_ref, prep_hbm, out_sem.at[1])
        occ_out.start()
        prep_out.start()
        return occ_out, prep_out

    def finish(p):
        off, size = PARTS[p]
        home = pl.ds(pl.multiple_of(me * wide + off, 512), size)
        h_all[:, home] = (x_all[:, home].astype(F32) + acc[:, off:off + size]).astype(BF16)
        if p == 0:
            h_far(0).start()
        h_near(p).start()

    o_near(0).wait_recv()
    p_dot(0, 0, 2)
    for i in range(8):
        p_copy(2, i).start()
    occ_out, prep_out = routing()
    o_far(0).wait_recv()
    o_pass(0).start()
    o_near(1).wait_recv()
    o_near(2).wait_recv()
    p_dot(0, 4, 2)
    o_pass(0).wait_recv()
    p_dot(0, 2, 2)
    p_dot(1, 0, 2)
    o_far(1).wait_recv()
    o_pass(1).start()
    p_dot(1, 2, 4)
    o_far(2).wait_recv()
    o_pass(2).start()
    p_dot(0, 6, 1, 2)
    p_dot(1, 6, 1, 2)
    o_pass(1).wait_recv()
    o_pass(2).wait_recv()
    p_dot(0, 7, 1, 0)
    finish(0)
    p_dot(1, 7, 1, 0)
    finish(1)
    p_dot(2, 0, 2)
    p_dot(2, 2, 4)
    p_dot(2, 6, 1)
    p_dot(2, 7, 1)
    finish(2)

    h_far(0).wait_recv()
    h_pass(0).start()
    whole = h_all.at[:, pl.ds(0, wide)]
    remote(whole, whole, x_snd, hd_rcv, core_mate).wait_recv()
    for core in range(2):
        rest = wide - HEAD
        cut = pl.ds(pl.multiple_of((me // 2 * 2 + core) * wide + HEAD, 512), rest)
        pltpu.make_async_copy(h_all.at[:, cut], tail_hbm.at[:, pl.ds(core * rest, rest)], out_sem.at[3]).start()
    h_pass(0).wait_recv()
    for dev in range(4):
        pltpu.make_async_copy(h_all.at[:, pl.ds(dev * wide, HEAD)], head_hbm.at[:, pl.ds(dev * HEAD, HEAD)],
                              out_sem.at[2]).start()

    remote(m_all.at[pl.ds(0, 3 * tok)], m_all.at[pl.ds(0, 3 * tok)], m_snd, m_rcv, core_mate).wait_send()
    sent = (3 * tok * width + 6 * seq * wide + seq * wide + 2 * seq * HEAD) // 1024
    sends = ring.at[pl.ds(0, sent), pl.ds(0, 1024)]
    remote(sends, sends, x_snd, hs_rcv, core_mate).wait_send()
    occ_out.wait()
    prep_out.wait()
    pltpu.make_async_copy(h_all.at[:, pl.ds(0, 2 * (wide - HEAD))], tail_hbm, out_sem.at[3]).wait()
    pltpu.make_async_copy(h_all.at[:, pl.ds(0, 4 * HEAD)], head_hbm, out_sem.at[2]).wait()


def attend(x, ids_t, probs, w_q, w_k, w_v, w_o, group):
    tok, width = x.shape
    seq = tok * group
    kv_w = w_k.shape[1] // group
    kv_dev = kv_w // HEAD_DIM
    wide = w_q.shape[1] // group // kv_dev
    steps = width // wide
    dma = pltpu.SemaphoreType.DMA
    parts = len(PARTS)
    assert steps == 4 and kv_dev == 2 and group == 4
    return pl.pallas_call(
        attend_kernel,
        out_shape=(jax.ShapeDtypeStruct((seq, 4 * HEAD), BF16), jax.ShapeDtypeStruct((seq, 2 * (wide - HEAD)), BF16),
                   jax.ShapeDtypeStruct((1, OCC), jnp.int32),
                   jax.ShapeDtypeStruct((8, seq), F32)),
        in_specs=[ANY] * 7,
        out_specs=(ANY, ANY, ANY, ANY),
        scratch_shapes=[
            pltpu.VMEM((SLOTS * wide, wide), BF16),
            pltpu.VMEM((width, 2 * kv_w), BF16),
            pltpu.VMEM((seq, width), BF16),
            pltpu.VMEM((seq, 2 * group * wide), BF16),
            pltpu.VMEM((seq, HEAD_DIM), F32),
            pltpu.VMEM((seq, width), BF16),
            pltpu.VMEM((seq, wide), F32),
            pltpu.VMEM((seq, 2 * kv_w), F32),
            pltpu.VMEM((seq, wide), BF16),
            pltpu.VMEM((seq, 2 * kv_w), BF16),
            pltpu.VMEM(x.shape, BF16), pltpu.VMEM(ids_t.shape, jnp.int32), pltpu.VMEM(probs.shape, F32),
            pltpu.VMEM((1, OCC), jnp.int32), pltpu.VMEM((8, seq), F32),
            dma((8,)), dma((11,)), dma((3,)), dma((4,)),
            dma, dma((steps,)), dma((steps,)), dma((3,)), dma((3,)), dma((3,)), dma, dma, dma, dma, dma],
        compiler_params=pltpu.CompilerParams(
            collective_id=0, has_side_effects=True, vmem_limit_bytes=66_000_000),
        cost_estimate=pl.CostEstimate(flops=seq * 2 * width * wide * 4, bytes_accessed=82_000_000, transcendentals=0),
        name='attend',
    )(x, ids_t, probs, w_q, w_k, w_v, w_o)


def zero_kernel(occ_hbm, buf_hbm, list_hbm, occ_ref, list_ref, zero, e_sem, z_sem, io_sem):
    experts = buf_hbm.shape[0]
    tok = buf_hbm.shape[1] // 4
    occ_copy = pltpu.make_async_copy(occ_hbm, occ_ref, io_sem.at[0])
    list_copy = pltpu.make_async_copy(list_ref, list_hbm, io_sem.at[1])
    occ_copy.start()
    zero[...] = jnp.zeros_like(zero)
    lax.fori_loop(0, BLIND, lambda e, c: (pltpu.make_async_copy(zero, buf_hbm.at[e], e_sem).start(), c)[1], 0)
    occ_copy.wait()

    def fill(e, wait):
        ones = [occ_ref[0, e * 4 + i] for i in range(4)]
        used = ones[0] + ones[1] + ones[2] + ones[3]

        def move(src, dst):
            copy = pltpu.make_async_copy(src, dst, z_sem)
            copy.wait() if wait else copy.start()

        @pl.when(used == 0)
        def _():
            move(zero, buf_hbm.at[e])

        @pl.when(used != 0)
        def _():
            for i in range(4):
                @pl.when(ones[i] == 0)
                def _():
                    move(zero.at[pl.ds(0, tok)], buf_hbm.at[e, pl.ds(i * tok, tok)])

    lax.fori_loop(BLIND, ZERO_FIRST, lambda e, c: (fill(e, False), c)[1], 0)

    def expert(e, count):
        for i in range(4):
            one = occ_ref[0, e * 4 + i]

            @pl.when(one != 0)
            def _():
                list_ref[0, count] = e * 4 + i
            count = count + one
        return count

    list_ref[0, OCC - 1] = lax.fori_loop(0, experts, expert, 0)
    list_copy.start()
    filled = buf_hbm.at[pl.ds(0, BLIND)]
    pltpu.make_async_copy(filled, filled, e_sem).wait()
    lax.fori_loop(BLIND, ZERO_FIRST, lambda e, c: (fill(e, True), c)[1], 0)
    list_copy.wait()


def zero_most(occ, experts, seq, width):
    dma = pltpu.SemaphoreType.DMA
    return pl.pallas_call(
        zero_kernel,
        out_shape=(jax.ShapeDtypeStruct((experts, seq, width), BF16), jax.ShapeDtypeStruct((1, OCC), jnp.int32)),
        in_specs=[ANY],
        out_specs=(ANY, ANY),
        scratch_shapes=[pltpu.SMEM((1, OCC), jnp.int32), pltpu.SMEM((1, OCC), jnp.int32), pltpu.VMEM((seq, width), BF16),
                        dma, dma, dma((2,))],
        compiler_params=pltpu.CompilerParams(vmem_limit_bytes=67_043_328),
        cost_estimate=pl.CostEstimate(flops=8_000_000_000, bytes_accessed=ZERO_FIRST * seq * width * 2, transcendentals=0),
        name='zero_most',
    )(occ)


def dispatch_kernel(list_hbm, occ_hbm, prep_hbm, head_hbm, tail_hbm, far_hbm, buf_in, buf_hbm, out_hbm, list_ref, occ_ref,
                    h, prep_ref, zero, stage, e_sem, z_sem, p_sem, io_sem, h_sem):
    me = lax.axis_index('sp')
    experts, seq, width = buf_hbm.shape
    tok = out_hbm.shape[0]
    wide = width // 4
    rest = wide - HEAD
    settled = ZERO_FIRST + EARLY
    list_copy = pltpu.make_async_copy(list_hbm, list_ref, io_sem.at[0])
    occ_copy = pltpu.make_async_copy(occ_hbm, occ_ref, io_sem.at[1])
    prep_copy = pltpu.make_async_copy(prep_hbm, prep_ref, io_sem.at[2])
    out_copy = pltpu.make_async_copy(h.at[span(me * tok, tok)], out_hbm, io_sem.at[3])
    list_copy.start()
    occ_copy.start()
    prep_copy.start()
    for dev in range(4):
        pltpu.make_async_copy(head_hbm.at[:, pl.ds(dev * HEAD, HEAD)], h.at[:, pl.ds(dev * wide, HEAD)], h_sem).start()
    for chip, src in ((me // 2, tail_hbm), (1 - me // 2, far_hbm)):
        for core in range(2):
            cut = pl.ds(pl.multiple_of((chip * 2 + core) * wide + HEAD, 512), rest)
            pltpu.make_async_copy(src.at[:, pl.ds(core * rest, rest)], h.at[:, cut], h_sem).start()
    zero[...] = jnp.zeros_like(zero)
    lax.fori_loop(ZERO_FIRST, settled, lambda e, c: (pltpu.make_async_copy(zero, buf_hbm.at[e], e_sem).start(), c)[1], 0)
    list_copy.wait()
    occ_copy.wait()

    def place(b):
        return buf_hbm.at[b // 4, span(lax.rem(b, 4) * tok, tok)]

    def fill(e, carry):
        ones = [occ_ref[0, e * 4 + i] for i in range(4)]
        used = ones[0] + ones[1] + ones[2] + ones[3]

        @pl.when(used == 0)
        def _():
            pltpu.make_async_copy(zero, buf_hbm.at[e], z_sem).start()

        @pl.when(used != 0)
        def _():
            for i in range(4):
                @pl.when(ones[i] == 0)
                def _():
                    pltpu.make_async_copy(zero.at[pl.ds(0, tok)], place(e * 4 + i), z_sem).start()
        return carry

    lax.fori_loop(settled, experts, fill, 0)
    count = list_ref[0, OCC - 1]
    prep_copy.wait()
    pltpu.make_async_copy(buf_hbm.at[0], h, h_sem).wait()
    out_copy.start()
    row = lax.broadcasted_iota(jnp.int32, (BLOCKS * tok, 1), 0)

    def batch_step(batch, carry):
        at = batch * BLOCKS
        key = jnp.zeros((BLOCKS * tok, 1), jnp.int32)
        for i in range(BLOCKS):
            key = jnp.where(row // tok == i, list_ref[0, at + i], key)
        key = ((key + me * experts * 4) * tok + lax.rem(row, tok)).astype(F32)
        hit0 = key == prep_ref[0:1, :]
        hit1 = key == prep_ref[1:2, :]
        gate = jnp.sum(jnp.where(hit0, prep_ref[2:3, :], 0.0) + jnp.where(hit1, prep_ref[3:4, :], 0.0),
                       axis=1, keepdims=True)
        pick = jnp.where(hit0 | hit1, 1.0, 0.0).astype(BF16)
        rows = (gate * dot(pick, h[...])).astype(BF16)
        for i in range(BLOCKS):
            stage[at + i] = rows[i * tok:(i + 1) * tok]

        @pl.when(batch == 0)
        def _():
            early = buf_hbm.at[pl.ds(ZERO_FIRST, EARLY)]
            pltpu.make_async_copy(early, early, e_sem).wait()

        for i in range(BLOCKS):
            b = list_ref[0, at + i]

            @pl.when((at + i < count) & (b < settled * 4))
            def _():
                pltpu.make_async_copy(stage.at[at + i], place(b), p_sem).start()

            @pl.when((at + i < count) & (b >= settled * 4))
            def _():
                pltpu.make_async_copy(stage.at[at + i], place(b), z_sem).start()
        return carry

    lax.fori_loop(0, jnp.maximum((count + BLOCKS - 1) // BLOCKS, 1), batch_step, 0)

    def landed(i, carry):
        @pl.when(list_ref[0, i] < settled * 4)
        def _():
            pltpu.make_async_copy(stage.at[0], place(0), p_sem).wait()
        return carry

    lax.fori_loop(0, count, landed, 0)
    others = buf_hbm.at[pl.ds(settled, experts - settled)]
    pltpu.make_async_copy(others, others, z_sem).wait()
    out_copy.wait()


def dispatch(blocks, occ, prep, head, tail, far, buf, tok):
    experts, seq, width = buf.shape
    dma = pltpu.SemaphoreType.DMA
    return pl.pallas_call(
        dispatch_kernel,
        out_shape=(jax.ShapeDtypeStruct(buf.shape, BF16), jax.ShapeDtypeStruct((tok, width), BF16)),
        in_specs=[ANY] * 7,
        out_specs=(ANY, ANY),
        input_output_aliases={6: 0},
        scratch_shapes=[pltpu.SMEM((1, OCC), jnp.int32), pltpu.SMEM((1, OCC), jnp.int32),
                        pltpu.VMEM((seq, width), BF16), pltpu.VMEM((8, seq), F32), pltpu.VMEM((seq, width), BF16),
                        pltpu.VMEM((experts * 4, tok, width), BF16), dma, dma, dma, dma((4,)), dma],
        compiler_params=pltpu.CompilerParams(vmem_limit_bytes=66_000_000),
        cost_estimate=pl.CostEstimate(flops=4_000_000_000, bytes_accessed=experts * seq * width, transcendentals=0),
        name='dispatch',
    )(blocks, occ, prep, head, tail, far, buf)


def solution(mesh):
    group = mesh.shape['sp']
    row_spec = P(('dp', 'sp'), None)
    buf_spec = P(('dp', 'sp'), None, None)

    def device_step(x_loc, w_q, w_k, w_v, w_o, ids_loc, probs_loc):
        head, tail, occ, prep = attend(x_loc, ids_loc.T, probs_loc, w_q, w_k, w_v, w_o, group)
        far = lax.ppermute(tail, 'sp', [(i, (i + 2) % group) for i in range(group)])
        buf, blocks = zero_most(occ, probs_loc.shape[1] // group, head.shape[0], x_loc.shape[1])
        buf, hidden_out = dispatch(blocks, occ, prep, head, tail, far, buf, x_loc.shape[0])
        return hidden_out, buf

    return jax.shard_map(device_step, mesh=mesh, in_specs=(row_spec, P(), P(), P(), P(), row_spec, row_spec), out_specs=(row_spec, buf_spec), check_vma=False)
```

```python
import math
import jax
import jax.numpy as jnp
from jax import lax
from jax.experimental import pallas as pl
from jax.experimental.pallas import tpu as pltpu
from jax.sharding import PartitionSpec as P

HEAD_DIM = 128
SCORE_SCALE = 1.0 / math.sqrt(HEAD_DIM)
SLOTS = 10
PARTS = ((0, 512), (512, 512), (1024, 512))
HEAD = 512
SEGS = ((0, 1536), (0, 1024), (1024, 512))
EARLY = 3
ZERO_FIRST = 30
BLIND = 4
BLOCKS = 8
OCC = 256
PLACE = (8, 9, 0, 1, 2, 3, 4, 5)
MESH = pl.DeviceIdType.MESH
ANY = pl.BlockSpec(memory_space=pl.ANY)
VMEM = pl.BlockSpec(memory_space=pltpu.VMEM)
SMEM = pl.BlockSpec(memory_space=pltpu.SMEM)
F32, BF16 = jnp.float32, jnp.bfloat16


def peer_of(me, mask):
    chip = lax.rem(me // 2 + mask // 2, 2)
    core = lax.rem(lax.rem(me, 2) + mask % 2, 2)
    return chip * 2 + core


def span(start, size):
    return pl.ds(pl.multiple_of(start, size), size)


def dot(a, b):
    return jnp.dot(a, b, preferred_element_type=F32)


def attend_kernel(x_hbm, ids_hbm, probs_hbm, wq_hbm, wk_hbm, wv_hbm, wo_hbm, head_hbm, tail_hbm, occ_hbm, prep_hbm,
                  ring, kv_buf, x_all, o_all, m_all, h_all, acc, kv_acc, q_ref, kv_ref, x_ref, ids_ref, probs_ref,
                  occ_ref, prep_ref, w_sem, p_sem, in_sem, out_sem, x_snd, xs_rcv, xd_rcv, os_rcv, od_rcv, of_rcv,
                  hs_rcv, hd_rcv, hf_rcv, m_snd, m_rcv):
    me = lax.axis_index('sp')
    tok, width = x_ref.shape
    seq = x_all.shape[0]
    wide = ring.shape[1]
    steps = width // wide
    kv_w = kv_buf.shape[1] // 2
    heads = wide // HEAD_DIM
    experts = probs_ref.shape[1] // 4
    core_mate = peer_of(me, 1)
    chip_mate = peer_of(me, 2)
    mine = span(me * tok, tok)
    theirs = span(chip_mate * tok, tok)

    def q_copy(c):
        rows = span(c * wide, wide)
        return pltpu.make_async_copy(wq_hbm.at[rows, span(me * 2 * wide, wide)], ring.at[rows], w_sem.at[c])

    def r_copy(seg, c):
        off, size = SEGS[seg]
        cols = pl.ds(pl.multiple_of((me * 2 + 1) * wide + off, 512), size)
        return pltpu.make_async_copy(wq_hbm.at[span(c * wide, wide), cols],
                                     ring.at[span((c + 4) * wide, wide), pl.ds(off, size)], w_sem.at[2 + 2 * seg + c // 2])

    def r_dot(seg, half):
        off, size = SEGS[seg]
        deep = 2 * wide
        base = 4 * wide + half * deep
        pltpu.make_async_copy(wq_hbm.at[pl.ds(0, deep), pl.ds(0, size)], ring.at[pl.ds(base, deep), pl.ds(off, size)],
                              w_sem.at[2 + 2 * seg + half]).wait()
        return dot(x_all[:, half * deep:(half + 1) * deep], ring[base:base + deep, off:off + size])

    def k_copy(c):
        rows = span(c * wide, wide)
        return pltpu.make_async_copy(wk_hbm.at[rows, span(me * kv_w, kv_w)], kv_buf.at[rows, pl.ds(0, kv_w)], w_sem.at[c])

    def v_copy(c):
        rows = span(c * wide, wide)
        return pltpu.make_async_copy(wv_hbm.at[rows, span(me * kv_w, kv_w)], kv_buf.at[rows, pl.ds(kv_w, kv_w)], w_sem.at[c])

    def p_sem_at(p, i):
        return i // 2 if p == 0 else 4 + (i + 2) // 4 if p == 1 else 7 + (i + 2) // 4 + i // 7

    def p_copy(p, i):
        off, size = PARTS[p]
        return pltpu.make_async_copy(
            wo_hbm.at[span((peer_of(me, i % 4) * 2 + i // 4) * wide, wide), pl.ds(pl.multiple_of(me * wide + off, 128), size)],
            ring.at[pl.ds(PLACE[i] * wide, wide), pl.ds(off, size)], p_sem.at[p_sem_at(p, i)])

    def p_dot(p, i, count, waits=None):
        off, size = PARTS[p]
        waits = count if waits is None else waits
        if waits:
            tile = ring.at[pl.ds(PLACE[i] * wide, waits * wide), pl.ds(off, size)]
            pltpu.make_async_copy(wo_hbm.at[pl.ds(0, waits * wide), pl.ds(0, size)], tile, p_sem.at[p_sem_at(p, i)]).wait()
        base = PLACE[i] * wide
        part = dot(o_all[:, i * wide:(i + count) * wide], ring[base:base + count * wide, off:off + size])
        if i == 0:
            acc[:, off:off + size] = part
        else:
            acc[:, off:off + size] += part

    def remote(src, dst, snd, rcv, to):
        return pltpu.make_async_remote_copy(src_ref=src, dst_ref=dst, send_sem=snd, recv_sem=rcv,
                                            device_id={'sp': to}, device_id_type=MESH)

    def x_far(c):
        cols = pl.ds(c * wide, wide)
        return remote(x_ref.at[:, cols], x_all.at[mine, cols], x_snd, xs_rcv.at[c], chip_mate)

    def x_near(c):
        cols = pl.ds(c * wide, wide)
        return remote(x_ref.at[:, cols], x_all.at[mine, cols], x_snd, xd_rcv.at[c], core_mate)

    def x_pass(c):
        cols = pl.ds(c * wide, wide)
        return remote(x_all.at[theirs, cols], x_all.at[theirs, cols], x_snd, xd_rcv.at[c], core_mate)

    def o_part(seg, r):
        off, size = SEGS[seg]
        return o_all.at[:, pl.ds((min(seg, 1) * 4 + r) * wide + off, size)]

    def o_far(seg):
        return remote(o_part(seg, 0), o_part(seg, 2), x_snd, os_rcv.at[seg], chip_mate)

    def o_near(seg):
        return remote(o_part(seg, 0), o_part(seg, 1), x_snd, od_rcv.at[seg], core_mate)

    def o_pass(seg):
        return remote(o_part(seg, 2), o_part(seg, 3), x_snd, of_rcv.at[seg], core_mate)

    def h_part(p, dev):
        off, size = PARTS[p]
        return h_all.at[:, pl.ds(pl.multiple_of(dev * wide + off, 128), size)]

    def h_far(p):
        return remote(h_part(p, me), h_part(p, me), x_snd, hs_rcv, chip_mate)

    def h_near(p):
        return remote(h_part(p, me), h_part(p, me), x_snd, hd_rcv, core_mate)

    def h_pass(p):
        return remote(h_part(p, chip_mate), h_part(p, chip_mate), x_snd, hf_rcv, core_mate)

    def m_send(mask):
        return remote(m_all.at[mine], m_all.at[mine], m_snd, m_rcv, peer_of(me, mask))

    barrier = pltpu.get_barrier_semaphore()
    for mask in (1, 2, 3):
        pl.semaphore_signal(barrier, inc=1, device_id={'sp': peer_of(me, mask)}, device_id_type=MESH)
    x_in = pltpu.make_async_copy(x_hbm, x_ref, in_sem.at[0])
    ids_in = pltpu.make_async_copy(ids_hbm, ids_ref, in_sem.at[1])
    probs_in = pltpu.make_async_copy(probs_hbm, probs_ref, in_sem.at[2])
    x_in.start()
    ids_in.start()
    probs_in.start()

    def start_first(c, carry):
        q_copy(c).start()
        k_copy(c).start()
        v_copy(c).start()
        return carry

    def start_second(c, carry):
        r_copy(1, c).start()
        return carry

    def start_third(c, carry):
        r_copy(2, c).start()
        return carry

    lax.fori_loop(0, 4, start_first, 0)
    lax.fori_loop(0, 4, start_second, 0)
    lax.fori_loop(0, 4, start_third, 0)
    p_copy(0, 0).start()
    p_copy(0, 1).start()
    x_in.wait()
    pl.semaphore_wait(barrier, 3)
    for c in range(steps):
        x_far(c).start()
        x_near(c).start()
    x_all[mine, :] = x_ref[...]
    ids_in.wait()
    probs_in.wait()
    ids = ids_ref[...].astype(F32)
    probs = probs_ref[...]
    eye = lax.broadcasted_iota(jnp.int32, (tok, tok), 0) == lax.broadcasted_iota(jnp.int32, (tok, tok), 1)
    id0 = jnp.sum(jnp.where(eye, ids[0:1, :], 0.0), axis=1, keepdims=True)
    id1 = jnp.sum(jnp.where(eye, ids[1:2, :], 0.0), axis=1, keepdims=True)
    lanes = lax.broadcasted_iota(jnp.int32, probs.shape, 1).astype(F32)
    p0 = jnp.sum(jnp.where(lanes == id0, probs, 0.0), axis=1, keepdims=True)
    p1 = jnp.sum(jnp.where(lanes == id1, probs, 0.0), axis=1, keepdims=True)
    total = p0 + p1
    cols = lax.broadcasted_iota(jnp.int32, (tok, HEAD_DIM), 1)
    m_all[mine, :] = jnp.where(cols == 0, id0, jnp.where(cols == 1, id1,
                     jnp.where(cols == 2, p0 / total, jnp.where(cols == 3, p1 / total, 0.0))))
    for mask in (1, 2, 3):
        m_send(mask).start()
    def first_dots(c):
        pair = x_all.at[pl.ds(0, 2 * tok), pl.ds(c * wide, wide)]
        remote(pair, pair, x_snd, xd_rcv.at[c], core_mate).wait_recv()
        chunk = pl.ds(0, wide + 2 * kv_w)
        pltpu.make_async_copy(wq_hbm.at[chunk, pl.ds(0, wide)], ring.at[chunk], w_sem.at[c]).wait()
        x = x_all[:, c * wide:(c + 1) * wide]
        part = dot(x, kv_buf[c * wide:(c + 1) * wide, :])
        if c == 0:
            kv_acc[...] = part
        else:
            kv_acc[...] += part
        part = dot(x, ring[c * wide:(c + 1) * wide, :])
        if c == 0:
            acc[...] = part
        else:
            acc[...] += part

    for c in range(steps):
        x_far(c).wait_recv()
        x_pass(c).start()
        if c > 0:
            first_dots(c - 1)
    first_dots(steps - 1)

    def attention(seg):
        kv = min(seg, 1)
        start, size = SEGS[seg]
        heads = size // HEAD_DIM
        k = kv_ref[:, kv * HEAD_DIM:(kv + 1) * HEAD_DIM]
        v = kv_ref[:, kv_w + kv * HEAD_DIM:kv_w + (kv + 1) * HEAD_DIM]
        cuts = [slice(start + m * HEAD_DIM, start + (m + 1) * HEAD_DIM) for m in range(heads)]
        q = jnp.concatenate([q_ref[:, c] for c in cuts], axis=0)
        s = lax.dot_general(q, k, (((1,), (1,)), ((), ())), preferred_element_type=F32) * SCORE_SCALE
        row = lax.rem(lax.broadcasted_iota(jnp.int32, s.shape, 0), seq)
        s = jnp.where(row >= lax.broadcasted_iota(jnp.int32, s.shape, 1), s, -1e30)
        e = jnp.exp(s - jnp.max(s, axis=1, keepdims=True))
        w = (e / jnp.sum(e, axis=1, keepdims=True)).astype(BF16)
        o = dot(w, v).astype(BF16)
        for m, c in enumerate(cuts):
            o_all[:, kv * 4 * wide + c.start:kv * 4 * wide + c.stop] = o[m * seq:(m + 1) * seq]
        o_far(seg).start()
        o_near(seg).start()

    kv_ref[...] = kv_acc[...].astype(BF16)
    q_ref[...] = acc[...].astype(BF16)
    for i in (2, 3, 4, 5):
        p_copy(0, i).start()
    attention(0)

    mid = SEGS[2][0]
    acc[:, :mid] = r_dot(1, 0)
    q_ref[:, :mid] = (acc[:, :mid] + r_dot(1, 1)).astype(BF16)
    attention(1)
    acc[:, mid:] = r_dot(2, 0)
    p_copy(0, 6).start()
    p_copy(0, 7).start()
    q_ref[:, mid:] = (acc[:, mid:] + r_dot(2, 1)).astype(BF16)
    for i in range(8):
        p_copy(1, i).start()
    attention(2)

    def routing():
        remote(m_all.at[pl.ds(0, 3 * tok)], m_all.at[pl.ds(0, 3 * tok)], m_snd, m_rcv, core_mate).wait_recv()
        meta = m_all[...]
        rows = meta.T
        t_col = lax.broadcasted_iota(jnp.int32, (seq, seq), 0)
        t_row = lax.broadcasted_iota(jnp.int32, (seq, seq), 1)
        before = (t_col < t_row) & (t_col // tok == t_row // tok)
        source = (lax.broadcasted_iota(jnp.int32, (1, seq), 1) // tok).astype(F32)
        for k in range(2):
            same = (meta[:, 0:1] == rows[k:k + 1, :]) | (meta[:, 1:2] == rows[k:k + 1, :])
            rank = jnp.sum(jnp.where(before & same, 1.0, 0.0), axis=0, keepdims=True)
            prep_ref[k:k + 1, :] = (rows[k:k + 1, :] * 4.0 + source) * tok + rank
        prep_ref[2:4, :] = rows[2:4, :]
        prep_ref[4:8, :] = jnp.zeros((4, seq), F32)
        block = (lax.broadcasted_iota(jnp.int32, (seq, OCC), 1) + me * experts * 4).astype(F32)
        origin = (lax.broadcasted_iota(jnp.int32, (seq, 1), 0) // tok).astype(F32)
        used = (meta[:, 0:1] * 4.0 + origin == block) | (meta[:, 1:2] * 4.0 + origin == block)
        occ_ref[...] = jnp.max(jnp.where(used, 1, 0), axis=0, keepdims=True)
        occ_out = pltpu.make_async_copy(occ_ref, occ_hbm, out_sem.at[0])
        prep_out = pltpu.make_async_copy(prep_ref, prep_hbm, out_sem.at[1])
        occ_out.start()
        prep_out.start()
        return occ_out, prep_out

    def finish(p):
        off, size = PARTS[p]
        home = pl.ds(pl.multiple_of(me * wide + off, 512), size)
        h_all[:, home] = (x_all[:, home].astype(F32) + acc[:, off:off + size]).astype(BF16)
        if p == 0:
            h_far(0).start()
        h_near(p).start()

    o_near(0).wait_recv()
    p_dot(0, 0, 2)
    for i in range(8):
        p_copy(2, i).start()
    occ_out, prep_out = routing()
    o_far(0).wait_recv()
    o_pass(0).start()
    o_near(1).wait_recv()
    o_near(2).wait_recv()
    p_dot(0, 4, 2)
    o_pass(0).wait_recv()
    p_dot(0, 2, 2)
    p_dot(1, 0, 2)
    o_far(1).wait_recv()
    o_pass(1).start()
    p_dot(1, 2, 4)
    o_far(2).wait_recv()
    o_pass(2).start()
    p_dot(0, 6, 1, 2)
    p_dot(1, 6, 1, 2)
    o_pass(1).wait_recv()
    o_pass(2).wait_recv()
    p_dot(0, 7, 1, 0)
    finish(0)
    p_dot(1, 7, 1, 0)
    finish(1)
    p_dot(2, 0, 2)
    p_dot(2, 2, 4)
    p_dot(2, 6, 1)
    p_dot(2, 7, 1)
    finish(2)

    h_far(0).wait_recv()
    h_pass(0).start()
    whole = h_all.at[:, pl.ds(0, wide)]
    remote(whole, whole, x_snd, hd_rcv, core_mate).wait_recv()
    for core in range(2):
        rest = wide - HEAD
        cut = pl.ds(pl.multiple_of((me // 2 * 2 + core) * wide + HEAD, 512), rest)
        pltpu.make_async_copy(h_all.at[:, cut], tail_hbm.at[:, pl.ds(core * rest, rest)], out_sem.at[3]).start()
    h_pass(0).wait_recv()
    for dev in range(4):
        pltpu.make_async_copy(h_all.at[:, pl.ds(dev * wide, HEAD)], head_hbm.at[:, pl.ds(dev * HEAD, HEAD)],
                              out_sem.at[2]).start()

    remote(m_all.at[pl.ds(0, 3 * tok)], m_all.at[pl.ds(0, 3 * tok)], m_snd, m_rcv, core_mate).wait_send()
    sent = (3 * tok * width + 6 * seq * wide + seq * wide + 2 * seq * HEAD) // 1024
    sends = ring.at[pl.ds(0, sent), pl.ds(0, 1024)]
    remote(sends, sends, x_snd, hs_rcv, core_mate).wait_send()
    occ_out.wait()
    prep_out.wait()
    pltpu.make_async_copy(h_all.at[:, pl.ds(0, 2 * (wide - HEAD))], tail_hbm, out_sem.at[3]).wait()
    pltpu.make_async_copy(h_all.at[:, pl.ds(0, 4 * HEAD)], head_hbm, out_sem.at[2]).wait()


def attend(x, ids_t, probs, w_q, w_k, w_v, w_o, group):
    tok, width = x.shape
    seq = tok * group
    kv_w = w_k.shape[1] // group
    kv_dev = kv_w // HEAD_DIM
    wide = w_q.shape[1] // group // kv_dev
    steps = width // wide
    dma = pltpu.SemaphoreType.DMA
    parts = len(PARTS)
    assert steps == 4 and kv_dev == 2 and group == 4
    return pl.pallas_call(
        attend_kernel,
        out_shape=(jax.ShapeDtypeStruct((seq, 4 * HEAD), BF16), jax.ShapeDtypeStruct((seq, 2 * (wide - HEAD)), BF16),
                   jax.ShapeDtypeStruct((1, OCC), jnp.int32),
                   jax.ShapeDtypeStruct((8, seq), F32)),
        in_specs=[ANY] * 7,
        out_specs=(ANY, ANY, ANY, ANY),
        scratch_shapes=[
            pltpu.VMEM((SLOTS * wide, wide), BF16),
            pltpu.VMEM((width, 2 * kv_w), BF16),
            pltpu.VMEM((seq, width), BF16),
            pltpu.VMEM((seq, 2 * group * wide), BF16),
            pltpu.VMEM((seq, HEAD_DIM), F32),
            pltpu.VMEM((seq, width), BF16),
            pltpu.VMEM((seq, wide), F32),
            pltpu.VMEM((seq, 2 * kv_w), F32),
            pltpu.VMEM((seq, wide), BF16),
            pltpu.VMEM((seq, 2 * kv_w), BF16),
            pltpu.VMEM(x.shape, BF16), pltpu.VMEM(ids_t.shape, jnp.int32), pltpu.VMEM(probs.shape, F32),
            pltpu.VMEM((1, OCC), jnp.int32), pltpu.VMEM((8, seq), F32),
            dma((8,)), dma((11,)), dma((3,)), dma((4,)),
            dma, dma((steps,)), dma((steps,)), dma((3,)), dma((3,)), dma((3,)), dma, dma, dma, dma, dma],
        compiler_params=pltpu.CompilerParams(
            collective_id=0, has_side_effects=True, vmem_limit_bytes=66_000_000),
        cost_estimate=pl.CostEstimate(flops=seq * 2 * width * wide * 4, bytes_accessed=82_000_000, transcendentals=0),
        name='attend',
    )(x, ids_t, probs, w_q, w_k, w_v, w_o)


def zero_kernel(occ_hbm, buf_hbm, list_hbm, occ_ref, list_ref, zero, e_sem, z_sem, io_sem):
    experts = buf_hbm.shape[0]
    tok = buf_hbm.shape[1] // 4
    occ_copy = pltpu.make_async_copy(occ_hbm, occ_ref, io_sem.at[0])
    list_copy = pltpu.make_async_copy(list_ref, list_hbm, io_sem.at[1])
    occ_copy.start()
    zero[...] = jnp.zeros_like(zero)
    lax.fori_loop(0, BLIND, lambda e, c: (pltpu.make_async_copy(zero, buf_hbm.at[e], e_sem).start(), c)[1], 0)
    occ_copy.wait()

    def fill(e, wait):
        ones = [occ_ref[0, e * 4 + i] for i in range(4)]
        used = ones[0] + ones[1] + ones[2] + ones[3]

        def move(src, dst):
            copy = pltpu.make_async_copy(src, dst, z_sem)
            copy.wait() if wait else copy.start()

        @pl.when(used == 0)
        def _():
            move(zero, buf_hbm.at[e])

        @pl.when(used != 0)
        def _():
            for i in range(4):
                @pl.when(ones[i] == 0)
                def _():
                    move(zero.at[pl.ds(0, tok)], buf_hbm.at[e, pl.ds(i * tok, tok)])

    lax.fori_loop(BLIND, ZERO_FIRST, lambda e, c: (fill(e, False), c)[1], 0)

    def expert(e, count):
        for i in range(4):
            one = occ_ref[0, e * 4 + i]

            @pl.when(one != 0)
            def _():
                list_ref[0, count] = e * 4 + i
            count = count + one
        return count

    list_ref[0, OCC - 1] = lax.fori_loop(0, experts, expert, 0)
    list_copy.start()
    filled = buf_hbm.at[pl.ds(0, BLIND)]
    pltpu.make_async_copy(filled, filled, e_sem).wait()
    lax.fori_loop(BLIND, ZERO_FIRST, lambda e, c: (fill(e, True), c)[1], 0)
    list_copy.wait()


def zero_most(occ, experts, seq, width):
    dma = pltpu.SemaphoreType.DMA
    return pl.pallas_call(
        zero_kernel,
        out_shape=(jax.ShapeDtypeStruct((experts, seq, width), BF16), jax.ShapeDtypeStruct((1, OCC), jnp.int32)),
        in_specs=[ANY],
        out_specs=(ANY, ANY),
        scratch_shapes=[pltpu.SMEM((1, OCC), jnp.int32), pltpu.SMEM((1, OCC), jnp.int32), pltpu.VMEM((seq, width), BF16),
                        dma, dma, dma((2,))],
        compiler_params=pltpu.CompilerParams(vmem_limit_bytes=67_043_328),
        cost_estimate=pl.CostEstimate(flops=8_000_000_000, bytes_accessed=ZERO_FIRST * seq * width * 2, transcendentals=0),
        name='zero_most',
    )(occ)


def dispatch_kernel(list_hbm, occ_hbm, prep_hbm, head_hbm, tail_hbm, far_hbm, buf_in, buf_hbm, out_hbm, list_ref, occ_ref,
                    h, prep_ref, zero, stage, e_sem, z_sem, p_sem, io_sem, h_sem):
    me = lax.axis_index('sp')
    experts, seq, width = buf_hbm.shape
    tok = out_hbm.shape[0]
    wide = width // 4
    rest = wide - HEAD
    settled = ZERO_FIRST + EARLY
    list_copy = pltpu.make_async_copy(list_hbm, list_ref, io_sem.at[0])
    occ_copy = pltpu.make_async_copy(occ_hbm, occ_ref, io_sem.at[1])
    prep_copy = pltpu.make_async_copy(prep_hbm, prep_ref, io_sem.at[2])
    out_copy = pltpu.make_async_copy(h.at[span(me * tok, tok)], out_hbm, io_sem.at[3])
    list_copy.start()
    occ_copy.start()
    prep_copy.start()
    for dev in range(4):
        pltpu.make_async_copy(head_hbm.at[:, pl.ds(dev * HEAD, HEAD)], h.at[:, pl.ds(dev * wide, HEAD)], h_sem).start()
    for chip, src in ((me // 2, tail_hbm), (1 - me // 2, far_hbm)):
        for core in range(2):
            cut = pl.ds(pl.multiple_of((chip * 2 + core) * wide + HEAD, 512), rest)
            pltpu.make_async_copy(src.at[:, pl.ds(core * rest, rest)], h.at[:, cut], h_sem).start()
    zero[...] = jnp.zeros_like(zero)
    lax.fori_loop(ZERO_FIRST, settled, lambda e, c: (pltpu.make_async_copy(zero, buf_hbm.at[e], e_sem).start(), c)[1], 0)
    list_copy.wait()
    occ_copy.wait()

    def place(b):
        return buf_hbm.at[b // 4, span(lax.rem(b, 4) * tok, tok)]

    def fill(e, carry):
        ones = [occ_ref[0, e * 4 + i] for i in range(4)]
        used = ones[0] + ones[1] + ones[2] + ones[3]

        @pl.when(used == 0)
        def _():
            pltpu.make_async_copy(zero, buf_hbm.at[e], z_sem).start()

        @pl.when(used != 0)
        def _():
            for i in range(4):
                @pl.when(ones[i] == 0)
                def _():
                    pltpu.make_async_copy(zero.at[pl.ds(0, tok)], place(e * 4 + i), z_sem).start()
        return carry

    lax.fori_loop(settled, experts, fill, 0)
    count = list_ref[0, OCC - 1]
    prep_copy.wait()
    pltpu.make_async_copy(buf_hbm.at[0], h, h_sem).wait()
    out_copy.start()
    row = lax.broadcasted_iota(jnp.int32, (BLOCKS * tok, 1), 0)

    def batch_step(batch, carry):
        at = batch * BLOCKS
        key = jnp.zeros((BLOCKS * tok, 1), jnp.int32)
        for i in range(BLOCKS):
            key = jnp.where(row // tok == i, list_ref[0, at + i], key)
        key = ((key + me * experts * 4) * tok + lax.rem(row, tok)).astype(F32)
        hit0 = key == prep_ref[0:1, :]
        hit1 = key == prep_ref[1:2, :]
        gate = jnp.sum(jnp.where(hit0, prep_ref[2:3, :], 0.0) + jnp.where(hit1, prep_ref[3:4, :], 0.0),
                       axis=1, keepdims=True)
        pick = jnp.where(hit0 | hit1, 1.0, 0.0).astype(BF16)
        rows = (gate * dot(pick, h[...])).astype(BF16)
        for i in range(BLOCKS):
            stage[at + i] = rows[i * tok:(i + 1) * tok]

        @pl.when(batch == 0)
        def _():
            early = buf_hbm.at[pl.ds(ZERO_FIRST, EARLY)]
            pltpu.make_async_copy(early, early, e_sem).wait()

        for i in range(BLOCKS):
            b = list_ref[0, at + i]

            @pl.when((at + i < count) & (b < settled * 4))
            def _():
                pltpu.make_async_copy(stage.at[at + i], place(b), p_sem).start()

            @pl.when((at + i < count) & (b >= settled * 4))
            def _():
                pltpu.make_async_copy(stage.at[at + i], place(b), z_sem).start()
        return carry

    lax.fori_loop(0, jnp.maximum((count + BLOCKS - 1) // BLOCKS, 1), batch_step, 0)

    def landed(i, carry):
        @pl.when(list_ref[0, i] < settled * 4)
        def _():
            pltpu.make_async_copy(stage.at[0], place(0), p_sem).wait()
        return carry

    lax.fori_loop(0, count, landed, 0)
    others = buf_hbm.at[pl.ds(settled, experts - settled)]
    pltpu.make_async_copy(others, others, z_sem).wait()
    out_copy.wait()


def dispatch(blocks, occ, prep, head, tail, far, buf, tok):
    experts, seq, width = buf.shape
    dma = pltpu.SemaphoreType.DMA
    return pl.pallas_call(
        dispatch_kernel,
        out_shape=(jax.ShapeDtypeStruct(buf.shape, BF16), jax.ShapeDtypeStruct((tok, width), BF16)),
        in_specs=[ANY] * 7,
        out_specs=(ANY, ANY),
        input_output_aliases={6: 0},
        scratch_shapes=[pltpu.SMEM((1, OCC), jnp.int32), pltpu.SMEM((1, OCC), jnp.int32),
                        pltpu.VMEM((seq, width), BF16), pltpu.VMEM((8, seq), F32), pltpu.VMEM((seq, width), BF16),
                        pltpu.VMEM((experts * 4, tok, width), BF16), dma, dma, dma, dma((4,)), dma],
        compiler_params=pltpu.CompilerParams(vmem_limit_bytes=66_000_000),
        cost_estimate=pl.CostEstimate(flops=4_000_000_000, bytes_accessed=experts * seq * width, transcendentals=0),
        name='dispatch',
    )(blocks, occ, prep, head, tail, far, buf)


def solution(mesh):
    group = mesh.shape['sp']
    row_spec = P(('dp', 'sp'), None)
    buf_spec = P(('dp', 'sp'), None, None)

    def device_step(x_loc, w_q, w_k, w_v, w_o, ids_loc, probs_loc):
        head, tail, occ, prep = attend(x_loc, ids_loc.T, probs_loc, w_q, w_k, w_v, w_o, group)
        far = lax.ppermute(tail, 'sp', [(i, (i + 2) % group) for i in range(group)])
        buf, blocks = zero_most(occ, probs_loc.shape[1] // group, head.shape[0], x_loc.shape[1])
        buf, hidden_out = dispatch(blocks, occ, prep, head, tail, far, buf, x_loc.shape[0])
        return hidden_out, buf

    return jax.shard_map(device_step, mesh=mesh, in_specs=(row_spec, P(), P(), P(), P(), row_spec, row_spec), out_specs=(row_spec, buf_spec), check_vma=False)
```
